32 devices in a mesh: dp: 16 (over z, y, x), mp: 2 (over core).
Axes of the slice: x: 2, y: 2, z: 4, core: 2. Of those that a mesh axis runs over, the one named last changes fastest.
Arguments:
- inputs: float32 [128, 197, 384], P('dp'), may hold values from -6 to 6
- cotangent: float32 [128, 197, 384], P('dp'), may hold values from -6 to 6
- first_gain: float32 [384], P('dp'), may hold values from 0.5 to 1.5
- first_shift: float32 [384], P('dp'), may hold values from -3 to 3
- mixer_weight: float32 [384, 3, 384], P('dp', None, 'mp'), may hold values from -6 to 6
- mixer_bias: float32 [2, 6, 64], P(None, 'mp', 'dp'), may hold values from -3 to 3
- output_weight: float32 [384, 384], P('mp', 'dp'), may hold values from -1.25 to 1.25
- output_bias: float32 [384], P('dp'), may hold values from -3 to 3
- second_gain: float32 [384], P('dp'), may hold values from 0.5 to 1.5
- second_shift: float32 [384], P('dp'), may hold values from -3 to 3
- expand_weight: float32 [384, 1536], P('dp', 'mp'), may hold values from -0.3125 to 0.3125
- expand_bias: float32 [24, 64], P('mp', 'dp'), may hold values from -3 to 3
- reduce_weight: float32 [1536, 384], P('mp', 'dp'), may hold values from -0.15625 to 0.15625
- reduce_bias: float32 [384], P('dp'), may hold values from -3 to 3
- momentum_first_gain: float32 [384], P('dp'), may hold values from -0.75 to 0.75
- momentum_first_shift: float32 [384], P('dp'), may hold values from -0.75 to 0.75
- momentum_mixer_weight: float32 [384, 3, 384], P('dp', None, 'mp'), may hold values from -0.75 to 0.75
- momentum_mixer_bias: float32 [2, 6, 64], P(None, 'mp', 'dp'), may hold values from -0.75 to 0.75
- momentum_output_weight: float32 [384, 384], P('mp', 'dp'), may hold values from -0.75 to 0.75
- momentum_output_bias: float32 [384], P('dp'), may hold values from -0.75 to 0.75
- momentum_second_gain: float32 [384], P('dp'), may hold values from -0.75 to 0.75
- momentum_second_shift: float32 [384], P('dp'), may hold values from -0.75 to 0.75
- momentum_expand_weight: float32 [384, 1536], P('dp', 'mp'), may hold values from -0.75 to 0.75
- momentum_expand_bias: float32 [24, 64], P('mp', 'dp'), may hold values from -0.75 to 0.75
- momentum_reduce_weight: float32 [1536, 384], P('mp', 'dp'), may hold values from -0.75 to 0.75
- momentum_reduce_bias: float32 [384], P('dp'), may hold values from -0.75 to 0.75
- variance_first_gain: float32 [384], P('dp'), may hold values from 0.0001 to 0.001
- variance_first_shift: float32 [384], P('dp'), may hold values from 0.0001 to 0.001
- variance_mixer_weight: float32 [384, 3, 384], P('dp', None, 'mp'), may hold values from 0.0001 to 0.001
- variance_mixer_bias: float32 [2, 6, 64], P(None, 'mp', 'dp'), may hold values from 0.0001 to 0.001
- variance_output_weight: float32 [384, 384], P('mp', 'dp'), may hold values from 0.0001 to 0.001
- variance_output_bias: float32 [384], P('dp'), may hold values from 0.0001 to 0.001
- variance_second_gain: float32 [384], P('dp'), may hold values from 0.0001 to 0.001
- variance_second_shift: float32 [384], P('dp'), may hold values from 0.0001 to 0.001
- variance_expand_weight: float32 [384, 1536], P('dp', 'mp'), may hold values from 0.0001 to 0.001
- variance_expand_bias: float32 [24, 64], P('mp', 'dp'), may hold values from 0.0001 to 0.001
- variance_reduce_weight: float32 [1536, 384], P('mp', 'dp'), may hold values from 0.0001 to 0.001
- variance_reduce_bias: float32 [384], P('dp'), may hold values from 0.0001 to 0.001
Outputs:
- block_out: float32 [128, 197, 384], P('dp')
- input_gradient: float32 [128, 197, 384], P('dp')
- gradient_first_gain: float32 [384], P('dp')
- gradient_first_shift: float32 [384], P('dp')
- gradient_mixer_weight: float32 [384, 3, 384], P('dp', None, 'mp')
- gradient_mixer_bias: float32 [2, 6, 64], P(None, 'mp', 'dp')
- gradient_output_weight: float32 [384, 384], P('mp', 'dp')
- gradient_output_bias: float32 [384], P('dp')
- gradient_second_gain: float32 [384], P('dp')
- gradient_second_shift: float32 [384], P('dp')
- gradient_expand_weight: float32 [384, 1536], P('dp', 'mp')
- gradient_expand_bias: float32 [24, 64], P('mp', 'dp')
- gradient_reduce_weight: float32 [1536, 384], P('mp', 'dp')
- gradient_reduce_bias: float32 [384], P('dp')
- updated_first_gain: float32 [384], P('dp')
- updated_first_shift: float32 [384], P('dp')
- updated_mixer_weight: float32 [384, 3, 384], P('dp', None, 'mp')
- updated_mixer_bias: float32 [2, 6, 64], P(None, 'mp', 'dp')
- updated_output_weight: float32 [384, 384], P('mp', 'dp')
- updated_output_bias: float32 [384], P('dp')
- updated_second_gain: float32 [384], P('dp')
- updated_second_shift: float32 [384], P('dp')
- updated_expand_weight: float32 [384, 1536], P('dp', 'mp')
- updated_expand_bias: float32 [24, 64], P('mp', 'dp')
- updated_reduce_weight: float32 [1536, 384], P('mp', 'dp')
- updated_reduce_bias: float32 [384], P('dp')
- updated_momentum_first_gain: float32 [384], P('dp')
- updated_momentum_first_shift: float32 [384], P('dp')
- updated_momentum_mixer_weight: float32 [384, 3, 384], P('dp', None, 'mp')
- updated_momentum_mixer_bias: float32 [2, 6, 64], P(None, 'mp', 'dp')
- updated_momentum_output_weight: float32 [384, 384], P('mp', 'dp')
- updated_momentum_output_bias: float32 [384], P('dp')
- updated_momentum_second_gain: float32 [384], P('dp')
- updated_momentum_second_shift: float32 [384], P('dp')
- updated_momentum_expand_weight: float32 [384, 1536], P('dp', 'mp')
- updated_momentum_expand_bias: float32 [24, 64], P('mp', 'dp')
- updated_momentum_reduce_weight: float32 [1536, 384], P('mp', 'dp')
- updated_momentum_reduce_bias: float32 [384], P('dp')
- updated_variance_first_gain: float32 [384], P('dp')
- updated_variance_first_shift: float32 [384], P('dp')
- updated_variance_mixer_weight: float32 [384, 3, 384], P('dp', None, 'mp')
- updated_variance_mixer_bias: float32 [2, 6, 64], P(None, 'mp', 'dp')
- updated_variance_output_weight: float32 [384, 384], P('mp', 'dp')
- updated_variance_output_bias: float32 [384], P('dp')
- updated_variance_second_gain: float32 [384], P('dp')
- updated_variance_second_shift: float32 [384], P('dp')
- updated_variance_expand_weight: float32 [384, 1536], P('dp', 'mp')
- updated_variance_expand_bias: float32 [24, 64], P('mp', 'dp')
- updated_variance_reduce_weight: float32 [1536, 384], P('mp', 'dp')
- updated_variance_reduce_bias: float32 [384], P('dp')
The draws below stay inside these ranges and needn't reach their ends.
All inputs are finite; a program needn't handle non-finite values.
Results may differ from the reference program's by a relative error of at most 0.0003.
Values sent between devices are 32-bit elements; how exact they have to be, the bound alone decides.
A program may use at most 192 MiB of HBM per device.

```python
import math
import jax
import jax.numpy as jnp
from jax import lax

D = 384
H = 6
HD = 64
FF = 1536
SEQ = 197
IMG_DEV = 8
IMAGES = 128
TOKENS = 25216
N_DP = 16


def draw_mixer_weight(key, part):
    first_key = jax.random.fold_in(key, 0)
    scale = D ** (-0.5)
    base = jnp.clip(jax.random.normal(first_key, (D, 3, D), jnp.float32), -6.0, 6.0) * scale
    return base


def block_levels(key, dims, cuts, least, high):
    level, own = 1.0, jax.random.fold_in(key, 6)
    for dim, parts in cuts:
        draws = jnp.exp(jax.random.uniform(jax.random.fold_in(own, dim), (parts,), jnp.float32, least / len(cuts), high / len(cuts)))
        level = level * jnp.repeat(draws, dims[dim] // parts).reshape([-1 if axis == dim else 1 for axis in range(len(dims))])
    return level


def centred(stream_key, extent, scale, most, cuts=(), held_as=jnp.bfloat16):
    entries = scale * jax.random.normal(stream_key, extent, jnp.float32)
    if cuts:
        entries = entries * block_levels(stream_key, extent, cuts, -0.22, 0.18)
    return jnp.clip(entries, -most, most).astype(held_as)


def setup_inputs(seed: int = 0) -> dict:
    arg_keys = jax.random.split(jax.random.key(seed), 39)
    inputs = centred(arg_keys[0], (IMAGES, SEQ, D), 1.0, 6.0, ((0, 16),), jnp.float32)
    cotangent = centred(arg_keys[1], (IMAGES, SEQ, D), 1.0, 6.0, ((0, 16),), jnp.float32)
    first_gain = jnp.clip(1.0 + 0.1 * jax.random.normal(arg_keys[2], (D,), jnp.float32), 0.5, 1.5)
    first_shift = centred(arg_keys[3], (D,), 0.5, 3.0, ((0, 16),), jnp.float32)
    mixer_weight = draw_mixer_weight(jax.random.fold_in(arg_keys[38], 71), 0)
    mixer_bias = centred(arg_keys[5], (2, H, HD), 0.5, 3.0, ((1, 2), (2, 16)), jnp.float32)
    output_weight = centred(arg_keys[6], (D, D), (D // 16) ** -0.5, 1.25, ((0, 2), (1, 16)), jnp.float32)
    output_bias = centred(arg_keys[7], (D,), 0.5, 3.0, ((0, 16),), jnp.float32)
    second_gain = jnp.clip(1.0 + 0.1 * jax.random.normal(arg_keys[8], (D,), jnp.float32), 0.5, 1.5)
    second_shift = centred(arg_keys[9], (D,), 0.5, 3.0, ((0, 16),), jnp.float32)
    expand_weight = centred(arg_keys[10], (D, FF), D ** -0.5, 0.3125, ((0, 16), (1, 2)), jnp.float32)
    expand_bias = centred(arg_keys[11], (FF // HD, HD), 0.5, 3.0, ((0, 2), (1, 16)), jnp.float32)
    reduce_weight = centred(arg_keys[12], (FF, D), FF ** -0.5, 0.15625, ((0, 2), (1, 16)), jnp.float32)
    reduce_bias = centred(arg_keys[13], (D,), 0.5, 3.0, ((0, 16),), jnp.float32)
    momentum_first_gain = centred(arg_keys[14], (D,), 0.05, 0.75, ((0, 16),), jnp.float32)
    momentum_first_shift = centred(arg_keys[15], (D,), 0.05, 0.75, ((0, 16),), jnp.float32)
    momentum_mixer_weight = centred(arg_keys[16], (D, 3, D), 0.05, 0.75, ((0, 16), (2, 2)), jnp.float32)
    momentum_mixer_bias = centred(arg_keys[17], (2, H, HD), 0.05, 0.75, ((1, 2), (2, 16)), jnp.float32)
    momentum_output_weight = centred(arg_keys[18], (D, D), 0.05, 0.75, ((0, 2), (1, 16)), jnp.float32)
    momentum_output_bias = centred(arg_keys[19], (D,), 0.05, 0.75, ((0, 16),), jnp.float32)
    momentum_second_gain = centred(arg_keys[20], (D,), 0.05, 0.75, ((0, 16),), jnp.float32)
    momentum_second_shift = centred(arg_keys[21], (D,), 0.05, 0.75, ((0, 16),), jnp.float32)
    momentum_expand_weight = centred(arg_keys[22], (D, FF), 0.05, 0.75, ((0, 16), (1, 2)), jnp.float32)
    momentum_expand_bias = centred(arg_keys[23], (FF // HD, HD), 0.05, 0.75, ((0, 2), (1, 16)), jnp.float32)
    momentum_reduce_weight = centred(arg_keys[24], (FF, D), 0.05, 0.75, ((0, 2), (1, 16)), jnp.float32)
    momentum_reduce_bias = centred(arg_keys[25], (D,), 0.05, 0.75, ((0, 16),), jnp.float32)
    variance_first_gain = jnp.clip(jnp.exp(math.log(0.001) - 2.3025852 * jax.random.uniform(arg_keys[26], (D,), jnp.float32) ** block_levels(arg_keys[26], (D,), ((0, 16),), -0.2, 0.2)), 0.0001, 0.001)
    variance_first_shift = jnp.clip(jnp.exp(math.log(0.001) - 2.3025852 * jax.random.uniform(arg_keys[27], (D,), jnp.float32) ** block_levels(arg_keys[27], (D,), ((0, 16),), -0.2, 0.2)), 0.0001, 0.001)
    variance_mixer_weight = jnp.clip(jnp.exp(math.log(0.001) - 2.3025852 * jax.random.uniform(arg_keys[28], (D, 3, D), jnp.float32) ** block_levels(arg_keys[28], (D, 3, D), ((0, 16), (2, 2)), -0.2, 0.2)), 0.0001, 0.001)
    variance_mixer_bias = jnp.clip(jnp.exp(math.log(0.001) - 2.3025852 * jax.random.uniform(arg_keys[29], (2, H, HD), jnp.float32) ** block_levels(arg_keys[29], (2, H, HD), ((1, 2), (2, 16)), -0.2, 0.2)), 0.0001, 0.001)
    variance_output_weight = jnp.clip(jnp.exp(math.log(0.001) - 2.3025852 * jax.random.uniform(arg_keys[30], (D, D), jnp.float32) ** block_levels(arg_keys[30], (D, D), ((0, 2), (1, 16)), -0.2, 0.2)), 0.0001, 0.001)
    variance_output_bias = jnp.clip(jnp.exp(math.log(0.001) - 2.3025852 * jax.random.uniform(arg_keys[31], (D,), jnp.float32) ** block_levels(arg_keys[31], (D,), ((0, 16),), -0.2, 0.2)), 0.0001, 0.001)
    variance_second_gain = jnp.clip(jnp.exp(math.log(0.001) - 2.3025852 * jax.random.uniform(arg_keys[32], (D,), jnp.float32) ** block_levels(arg_keys[32], (D,), ((0, 16),), -0.2, 0.2)), 0.0001, 0.001)
    variance_second_shift = jnp.clip(jnp.exp(math.log(0.001) - 2.3025852 * jax.random.uniform(arg_keys[33], (D,), jnp.float32) ** block_levels(arg_keys[33], (D,), ((0, 16),), -0.2, 0.2)), 0.0001, 0.001)
    variance_expand_weight = jnp.clip(jnp.exp(math.log(0.001) - 2.3025852 * jax.random.uniform(arg_keys[34], (D, FF), jnp.float32) ** block_levels(arg_keys[34], (D, FF), ((0, 16), (1, 2)), -0.2, 0.2)), 0.0001, 0.001)
    variance_expand_bias = jnp.clip(jnp.exp(math.log(0.001) - 2.3025852 * jax.random.uniform(arg_keys[35], (FF // HD, HD), jnp.float32) ** block_levels(arg_keys[35], (FF // HD, HD), ((0, 2), (1, 16)), -0.2, 0.2)), 0.0001, 0.001)
    variance_reduce_weight = jnp.clip(jnp.exp(math.log(0.001) - 2.3025852 * jax.random.uniform(arg_keys[36], (FF, D), jnp.float32) ** block_levels(arg_keys[36], (FF, D), ((0, 2), (1, 16)), -0.2, 0.2)), 0.0001, 0.001)
    variance_reduce_bias = jnp.clip(jnp.exp(math.log(0.001) - 2.3025852 * jax.random.uniform(arg_keys[37], (D,), jnp.float32) ** block_levels(arg_keys[37], (D,), ((0, 16),), -0.2, 0.2)), 0.0001, 0.001)
    return dict(inputs=inputs, cotangent=cotangent, first_gain=first_gain, first_shift=first_shift, mixer_weight=mixer_weight, mixer_bias=mixer_bias, output_weight=output_weight, output_bias=output_bias, second_gain=second_gain, second_shift=second_shift, expand_weight=expand_weight, expand_bias=expand_bias, reduce_weight=reduce_weight, reduce_bias=reduce_bias, momentum_first_gain=momentum_first_gain, momentum_first_shift=momentum_first_shift, momentum_mixer_weight=momentum_mixer_weight, momentum_mixer_bias=momentum_mixer_bias, momentum_output_weight=momentum_output_weight, momentum_output_bias=momentum_output_bias, momentum_second_gain=momentum_second_gain, momentum_second_shift=momentum_second_shift, momentum_expand_weight=momentum_expand_weight, momentum_expand_bias=momentum_expand_bias, momentum_reduce_weight=momentum_reduce_weight, momentum_reduce_bias=momentum_reduce_bias, variance_first_gain=variance_first_gain, variance_first_shift=variance_first_shift, variance_mixer_weight=variance_mixer_weight, variance_mixer_bias=variance_mixer_bias, variance_output_weight=variance_output_weight, variance_output_bias=variance_output_bias, variance_second_gain=variance_second_gain, variance_second_shift=variance_second_shift, variance_expand_weight=variance_expand_weight, variance_expand_bias=variance_expand_bias, variance_reduce_weight=variance_reduce_weight, variance_reduce_bias=variance_reduce_bias)


norm_eps = 1e-06
beta_one = 0.9
beta_two = 0.99
adam_eps = 1e-08
learn_rate = 0.05
weight_decay = 0.05
step_count = 3.0

def layer_norm(values, gain, shift):
    center = values - lax.optimization_barrier(jnp.mean(values, axis=-1, keepdims=True))
    spread = lax.optimization_barrier(jnp.mean(center * center, axis=-1, keepdims=True))
    return center * lax.rsqrt(spread + norm_eps) * gain + shift

def forward(tokens, params):
    first_gain, first_shift, mixer_weight, mixer_bias, output_weight, output_bias, second_gain, second_shift, expand_weight, expand_bias, reduce_weight, reduce_bias = params
    highest = lax.Precision.HIGHEST
    images, length = (tokens.shape[0], tokens.shape[1])
    first_normed = layer_norm(tokens, first_gain, first_shift)
    mixed = jnp.einsum('bsd,dcf->bscf', first_normed, mixer_weight, precision=highest)
    query = (mixed[:, :, 0] + mixer_bias[0].reshape(-1)).reshape(images, length, H, HD)
    keys_all = mixed[:, :, 1].reshape(images, length, H, HD)
    values = (mixed[:, :, 2] + mixer_bias[1].reshape(-1)).reshape(images, length, H, HD)
    scores = jnp.einsum('bqhe,bkhe->bhqk', query, keys_all, precision=highest) * HD ** (-0.5)
    probs = jax.nn.softmax(scores, axis=-1)
    heads = jnp.einsum('bhqk,bkhe->bqhe', probs, values, precision=highest).reshape(images, length, D)
    middle = tokens + jnp.einsum('bsf,fd->bsd', heads, output_weight, precision=highest) + output_bias
    second_normed = layer_norm(middle, second_gain, second_shift)
    hidden = jnp.einsum('bsd,df->bsf', second_normed, expand_weight, precision=highest) + expand_bias.reshape(-1)
    active = jax.nn.gelu(hidden, approximate=False)
    return middle + jnp.einsum('bsf,fd->bsd', active, reduce_weight, precision=highest) + reduce_bias

def adam_update(param, grad, momentum, variance, decay):
    momentum_next = beta_one * momentum + (1.0 - beta_one) * grad
    variance_next = beta_two * variance + (1.0 - beta_two) * grad * grad
    mean_hat = momentum_next / (1.0 - beta_one ** step_count)
    square_hat = variance_next / (1.0 - beta_two ** step_count)
    stepped = param - learn_rate * (mean_hat / (jnp.sqrt(square_hat) + adam_eps) + decay * param)
    return (stepped, momentum_next, variance_next)

def reference(inputs, cotangent, first_gain, first_shift, mixer_weight, mixer_bias, output_weight, output_bias, second_gain, second_shift, expand_weight, expand_bias, reduce_weight, reduce_bias, momentum_first_gain, momentum_first_shift, momentum_mixer_weight, momentum_mixer_bias, momentum_output_weight, momentum_output_bias, momentum_second_gain, momentum_second_shift, momentum_expand_weight, momentum_expand_bias, momentum_reduce_weight, momentum_reduce_bias, variance_first_gain, variance_first_shift, variance_mixer_weight, variance_mixer_bias, variance_output_weight, variance_output_bias, variance_second_gain, variance_second_shift, variance_expand_weight, variance_expand_bias, variance_reduce_weight, variance_reduce_bias):
    params = (first_gain, first_shift, mixer_weight, mixer_bias, output_weight, output_bias, second_gain, second_shift, expand_weight, expand_bias, reduce_weight, reduce_bias)
    momenta = (momentum_first_gain, momentum_first_shift, momentum_mixer_weight, momentum_mixer_bias, momentum_output_weight, momentum_output_bias, momentum_second_gain, momentum_second_shift, momentum_expand_weight, momentum_expand_bias, momentum_reduce_weight, momentum_reduce_bias)
    variances = (variance_first_gain, variance_first_shift, variance_mixer_weight, variance_mixer_bias, variance_output_weight, variance_output_bias, variance_second_gain, variance_second_shift, variance_expand_weight, variance_expand_bias, variance_reduce_weight, variance_reduce_bias)
    token_blocks = inputs.reshape(N_DP, IMG_DEV, SEQ, D)
    incoming = cotangent.reshape(N_DP, IMG_DEV, SEQ, D)

    def one_block(totals, pair):
        block_in, block_cot = pair
        outputs, pullback = jax.vjp(forward, block_in, params)
        block_grad, param_grads = pullback(block_cot)
        totals = tuple((total + grad for total, grad in zip(totals, param_grads)))
        return (totals, (outputs, block_grad))
    zeros = tuple((jnp.zeros_like(param) for param in params))
    totals, (outputs, back) = lax.scan(one_block, zeros, (token_blocks, incoming))
    scale = TOKENS ** (-0.5)
    gradients = tuple((total * scale for total in totals))
    decays = (0.0, 0.0, weight_decay, 0.0, weight_decay, 0.0, 0.0, 0.0, weight_decay, 0.0, weight_decay, 0.0)
    results = [adam_update(p, g, m, v, w) for p, g, m, v, w in zip(params, gradients, momenta, variances, decays)]
    stepped = tuple((item[0] for item in results))
    moments = tuple((item[1] for item in results))
    squares = tuple((item[2] for item in results))
    return (outputs.reshape(IMAGES, SEQ, D), back.reshape(IMAGES, SEQ, D), *gradients, *stepped, *moments, *squares)
```

```python
import functools
import heapq

import jax
import jax.numpy as jnp
from jax import lax
from jax.experimental import pallas as pl
from jax.experimental.pallas import tpu as pltpu
from jax.sharding import PartitionSpec as P

norm_eps = 1e-06
beta_one = 0.9
beta_two = 0.99
adam_eps = 1e-08
learn_rate = 0.05
weight_decay = 0.05
step_count = 3.0

LANES = 128
MASKED = -1e30
f32, bf16 = jnp.float32, jnp.bfloat16


def split(x):
    high = x.astype(bf16)
    return high, (x - high.astype(f32)).astype(bf16)


def dot(a, b, da, db):
    return lax.dot_general(a, b, (((da,), (db,)), ((), ())), preferred_element_type=f32)


def product(a, b, da, db):
    left = jnp.concatenate([a[0], a[0], a[1]], axis=da)
    right = jnp.concatenate([b[0], b[1], b[0]], axis=db)
    return dot(left, right, da, db)


def product_apart(a, b, da, db):
    return dot(a[0], b[0], da, db) + dot(a[0], b[1], da, db) + dot(a[1], b[0], da, db)


def layer_kernel(length, heads, head, base, x_ref, cot_ref, w_ref, vec_ref, mb_ref, eb_ref,
                 y_ref, gx_ref, g_ref, sg_ref,
                 whi, wlo, wsem, pad, mixed, probs_hi, probs_lo, joined,
                 fo_hi, fo_lo, so_hi, so_lo, cot_hi, cot_lo, gm_hi, gm_lo, part, part2):
    step = pl.program_id(0)
    rows, width = pad.shape[1], pad.shape[2]
    local = heads * head
    qkv = 5 * LANES
    hidden_local = eb_ref.shape[-1]
    attn = 6 * LANES
    up, down, end = attn, attn + hidden_local, attn + 2 * hidden_local

    @pl.when(step == 0)
    def _():
        for c in range(2):
            pltpu.make_async_copy(w_ref.at[c], g_ref.at[c], wsem.at[c]).start()
        pad[...] = jnp.zeros_like(pad)
        sg_ref[...] = jnp.zeros_like(sg_ref)
        for c in range(2):
            pltpu.make_async_copy(w_ref.at[c], g_ref.at[c], wsem.at[c]).wait()

        def convert(t, _):
            c, r = t // (width // 16), t % (width // 16)
            at = pl.ds(pl.multiple_of(r * 16, 16), 16)
            high, low = split(g_ref[c, at, 0:end])
            whi[c, at, :] = high
            wlo[c, at, :] = low
            g_ref[c, at, :] = jnp.zeros((16, g_ref.shape[2]), f32)
            return 0

        lax.fori_loop(0, 2 * (width // 16), convert, 0)

    def weight(c, lo, hi):
        return whi[c, :, lo:hi], wlo[c, :, lo:hi]

    def vec(r):
        return vec_ref[r:r + 1, :]

    def normalize(v):
        center = v - jnp.mean(v, axis=-1, keepdims=True)
        inverse = lax.rsqrt(jnp.mean(center * center, axis=-1, keepdims=True) + norm_eps)
        return center * inverse, inverse

    def norm_back(grad, normed, inverse, gain):
        scaled = grad * gain
        return inverse * (scaled - jnp.mean(scaled, axis=-1, keepdims=True)
                          - normed * jnp.mean(scaled * normed, axis=-1, keepdims=True))

    def total(v):
        return jnp.sum(v, axis=0, keepdims=True)

    pad[0, 0:length, :] = x_ref[0]
    pad[1, 0:length, :] = cot_ref[0]
    x, cot = pad[0], pad[1]
    cot_hi[...], cot_lo[...] = split(cot)
    first, first_inverse = normalize(x)
    fo_hi[...], fo_lo[...] = split(first * vec(0) + vec(1))

    lane = lax.broadcasted_iota(jnp.int32, (rows, LANES), 1)
    sides = (lane < head, lane >= head)
    column = lax.broadcasted_iota(jnp.int32, (rows, rows), 1)
    score_scale = head ** (-0.5)

    def side(v, s):
        return jnp.where(sides[s], v, 0.0)

    def swap(v):
        return pltpu.roll(v, head, 1)

    def windows(c):
        w = [mixed[c, :, t * LANES:(t + 1) * LANES] for t in range(5)]
        third = side(w[3], 0) * score_scale, side(swap(w[3]), 0), side(w[4], 0)
        return [
            (side(w[0], 0) * score_scale, side(w[1], 0), side(w[2], 0)),
            (side(w[0], 1) * score_scale, side(w[1], 1), side(w[2], 1)),
            third,
        ]

    part[...] = jnp.zeros_like(part)

    def attend(c, _):
        mixed[c] = product((fo_hi[...], fo_lo[...]), weight(c, 0, qkv), 1, 0) + mb_ref[c]
        outs = []
        for h, (q, k, v) in enumerate(windows(c)):
            scores = product(split(q), split(k), 1, 1)
            scores = jnp.where(column < length, scores, MASKED)
            expon = jnp.exp(scores - jnp.max(scores, axis=-1, keepdims=True))
            probs = split(expon / jnp.sum(expon, axis=-1, keepdims=True))
            probs_hi[c, h], probs_lo[c, h] = probs
            outs.append(product_apart(probs, split(v), 1, 0))
        joined[c] = jnp.concatenate([swap(outs[2]), outs[0] + outs[1]], axis=1)
        part[...] += product(split(joined[c]), weight(c, 4 * LANES, attn), 1, 1)
        return 0

    lax.fori_loop(0, 2, attend, 0)
    middle = x + part[...] + vec(2)
    second, second_inverse = normalize(middle)
    so_hi[...], so_lo[...] = split(second * vec(3) + vec(4))

    part[...] = middle + vec(5)
    part2[...] = jnp.zeros_like(part2)

    def feed(c, _):
        so = (so_hi[...], so_lo[...])
        co = (cot_hi[...], cot_lo[...])
        hidden = product(so, weight(c, up, down), 1, 0) + eb_ref[c]
        share = 0.5 * (1.0 + lax.erf(hidden * (0.5 ** 0.5)))
        active = split(hidden * share)
        slope = share + hidden * jnp.exp(-0.5 * hidden * hidden) * 0.3989422804014327
        part[...] += product(active, weight(c, down, end), 1, 1)
        g_ref[c, :, down:end] += product(co, active, 0, 0)
        grad = product(co, weight(c, down, end), 1, 0) * slope
        sg_ref[c, 7:8, 0:hidden_local] += total(grad)
        grad = split(grad)
        g_ref[c, :, up:down] += product(so, grad, 0, 0)
        part2[...] += product(grad, weight(c, up, down), 1, 1)
        return 0

    lax.fori_loop(0, 2, feed, 0)
    y_ref[0] = part[0:length, :]

    grad_second = part2[...]
    sg_ref[0, 3:4, 0:width] += total(grad_second * second)
    sg_ref[0, 4:5, 0:width] += total(grad_second)
    sg_ref[0, 5:6, 0:width] += total(cot)
    grad_middle = cot + norm_back(grad_second, second, second_inverse, vec(3))
    sg_ref[0, 2:3, 0:width] += total(grad_middle)
    gm_hi[...], gm_lo[...] = split(grad_middle)
    part2[...] = grad_middle

    part[...] = jnp.zeros_like(part)

    def attend_back(c, _):
        gm = (gm_hi[...], gm_lo[...])
        fo = (fo_hi[...], fo_lo[...])
        grad_heads = product(gm, weight(c, 4 * LANES, attn), 1, 0)
        g_ref[c, :, 4 * LANES:attn] += product(gm, split(joined[c]), 0, 0)
        pair, single = grad_heads[:, LANES:], swap(grad_heads[:, :LANES])
        pair_out, single_out = joined[c, :, LANES:], swap(joined[c, :, :LANES])
        grad_outs = (side(pair, 0), side(pair, 1), side(single, 0))
        outs = (pair_out, pair_out, single_out)
        grads = []
        for h, (q, k, v) in enumerate(windows(c)):
            grad_out = grad_outs[h]
            row = jnp.sum(grad_out * outs[h], axis=-1, keepdims=True)
            grad_out = split(grad_out)
            grad_probs = product(grad_out, split(v), 1, 1)
            probs = (probs_hi[c, h], probs_lo[c, h])
            grad_v = product(probs, grad_out, 0, 0)
            grad_scores = split((probs[0].astype(f32) + probs[1].astype(f32)) * (grad_probs - row))
            grad_q = product_apart(grad_scores, split(k), 1, 0) * score_scale
            grad_k = product(grad_scores, split(q), 0, 0)
            grads.append((grad_q, grad_k, grad_v))
        one, two, three = grads
        grad_mixed = jnp.concatenate(
            [one[0] + two[0], one[1] + two[1], one[2] + two[2], three[0] + swap(three[1]), three[2]], axis=1)
        sg_ref[c, 6:7, 0:qkv] += total(grad_mixed)
        grad_mixed = split(grad_mixed)
        g_ref[c, :, 0:qkv] += product(fo, grad_mixed, 0, 0)
        part[...] += product(grad_mixed, weight(c, 0, qkv), 1, 1)
        return 0

    lax.fori_loop(0, 2, attend_back, 0)
    grad_first = part[...]
    sg_ref[0, 0:1, 0:width] += total(grad_first * first)
    sg_ref[0, 1:2, 0:width] += total(grad_first)
    gx_ref[0] = (part2[...] + norm_back(grad_first, first, first_inverse, vec(0)))[0:length, :]


def run_layer(base, inputs, cotangent, weights, vectors, mixed_bias, expand_bias, heads, head):
    images, length, width = inputs.shape
    own = images // 2
    rows = -(-length // 16) * 16
    columns = weights.shape[-1]
    hidden_local = expand_bias.shape[-1]
    end = 6 * LANES + 2 * hidden_local
    image = pl.BlockSpec((1, length, width), lambda i, b: (b[0] + i, 0, 0))

    def whole(shape):
        return pl.BlockSpec(shape, lambda i, b: (0,) * len(shape))

    act = pltpu.VMEM((rows, width), bf16)
    return pl.pallas_call(
        functools.partial(layer_kernel, length, heads, head),
        grid_spec=pltpu.PrefetchScalarGridSpec(
            num_scalar_prefetch=1,
            grid=(own,),
            in_specs=[image, image, pl.BlockSpec(memory_space=pl.ANY), whole(vectors.shape),
                      whole(mixed_bias.shape), whole(expand_bias.shape)],
            out_specs=[image, image, whole((2, width, columns)), whole((2, 8, hidden_local))],
            scratch_shapes=[
                pltpu.VMEM((2, width, end), bf16), pltpu.VMEM((2, width, end), bf16),
                pltpu.SemaphoreType.DMA((2,)),
                pltpu.VMEM((2, rows, width), f32),
                pltpu.VMEM((2, rows, 5 * LANES), f32),
                pltpu.VMEM((2, heads, rows, rows), bf16), pltpu.VMEM((2, heads, rows, rows), bf16),
                pltpu.VMEM((2, rows, 2 * LANES), f32),
                act, act, act, act, act, act, act, act,
                pltpu.VMEM((rows, width), f32), pltpu.VMEM((rows, width), f32),
            ],
        ),
        out_shape=[
            jax.ShapeDtypeStruct(inputs.shape, f32), jax.ShapeDtypeStruct(inputs.shape, f32),
            jax.ShapeDtypeStruct((2, width, columns), f32), jax.ShapeDtypeStruct((2, 8, hidden_local), f32),
        ],
        compiler_params=pltpu.CompilerParams(
            dimension_semantics=("arbitrary",), vmem_limit_bytes=60 * 2**20),
        name="layer",
    )(base, inputs, cotangent, weights, vectors, mixed_bias, expand_bias)


def rings(n):
    side = max(k for k in range(1, n + 1) if n % (k * k) == 0 and n // (k * k) >= k)
    return n // (side * side), side, side


def place(sizes):
    first, side, _ = sizes
    core, me = lax.axis_index("mp"), lax.axis_index("dp")
    a, b, c = me // (side * side), (me // side) % side, me % side

    def at(slab, sign=1, of=core):
        i, j, k = slab
        i, j, k = (sign * i) % first, (sign * j) % side, (sign * k) % side
        ahead_b = j * of + k * (1 - of)
        ahead_c = k * of + j * (1 - of)
        return (((a + i) % first) * side + (b + ahead_b) % side) * side + (c + ahead_c) % side

    return core, at


UNITS = ((1, 0, 0), (0, 1, 0), (0, 0, 1))


def plus(slab, unit):
    return tuple(s + u for s, u in zip(slab, unit))


def sends(slab, sizes):
    return [r for r in range(3) if not any(slab[r + 1:]) and slab[r] + 1 < sizes[r]]


def arrival_order(sizes):
    cost, free, heap, order = (2.0, 1.5, 1.5), [0.0] * 3, [(0.0, (0, 0, 0))], []
    while heap:
        now, slab = heapq.heappop(heap)
        order.append(slab)
        for r in sends(slab, sizes):
            free[r] = max(now, free[r]) + cost[r]
            heapq.heappush(heap, (free[r], plus(slab, UNITS[r])))
    return order


def slab_id(slab, sizes):
    return (slab[0] * sizes[1] + slab[1]) * sizes[2] + slab[2]


def greet(core, at, sign):
    barrier = pltpu.get_barrier_semaphore()
    for unit in UNITS:
        pl.semaphore_signal(barrier, inc=1, device_id={"dp": at(unit, sign)})
    pl.semaphore_signal(barrier, inc=1, device_id={"mp": 1 - core})
    pl.semaphore_wait(barrier, 4)


def gather_kernel(sizes, slab_ref, out_ref, send_sem, recv_sem, swap_send, swap_recv, own_sem):
    core, at = place(sizes)
    number = functools.partial(slab_id, sizes=sizes)
    greet(core, at, -1)

    def landing(slab, of):
        return out_ref.at[of, at(slab, -1, of)]

    started = []
    own = pltpu.make_async_copy(slab_ref, landing((0, 0, 0), core), own_sem)
    for slab in arrival_order(sizes):
        spot = landing(slab, core)
        if any(slab):
            pltpu.make_async_remote_copy(
                src_ref=spot, dst_ref=spot, send_sem=send_sem.at[0, 0], recv_sem=recv_sem.at[number(slab)],
                device_id={"mp": 1 - core}).wait_recv()
        source = spot if any(slab) else slab_ref
        for r in reversed(sends(slab, sizes)):
            copy = pltpu.make_async_remote_copy(
                src_ref=source, dst_ref=spot, send_sem=send_sem.at[r, number(slab)],
                recv_sem=recv_sem.at[number(plus(slab, UNITS[r]))], device_id={"dp": at(UNITS[r])})
            copy.start()
            started.append(copy)
        copy = pltpu.make_async_remote_copy(
            src_ref=source, dst_ref=spot, send_sem=swap_send.at[number(slab)], recv_sem=swap_recv.at[number(slab)],
            device_id={"mp": 1 - core})
        copy.start()
        started.append(copy)
        if not any(slab):
            own.start()
    for slab in arrival_order(sizes):
        spot = landing(slab, 1 - core)
        pltpu.make_async_remote_copy(
            src_ref=spot, dst_ref=spot, send_sem=swap_send.at[0], recv_sem=swap_recv.at[number(slab)],
            device_id={"mp": 1 - core}).wait_recv()
    for copy in started:
        copy.wait_send()
    own.wait()


def gather(slab, n):
    sizes = rings(n)
    return pl.pallas_call(
        functools.partial(gather_kernel, sizes),
        out_shape=jax.ShapeDtypeStruct((2, n) + slab.shape, f32),
        in_specs=[pl.BlockSpec(memory_space=pltpu.VMEM)],
        out_specs=pl.BlockSpec(memory_space=pl.ANY),
        scratch_shapes=[
            pltpu.SemaphoreType.DMA((3, n)), pltpu.SemaphoreType.DMA((n,)),
            pltpu.SemaphoreType.DMA((n,)), pltpu.SemaphoreType.DMA((n,)), pltpu.SemaphoreType.DMA,
        ],
        compiler_params=pltpu.CompilerParams(collective_id=0, has_side_effects=True),
        name="gather",
    )(slab)


def scatter_kernel(sizes, g_ref, y_in, gx_in, out_ref, y_ref, gx_ref,
                   acc, swapped, landed, load_sem, send_sem, recv_sem, swap_send, swap_recv, image_send, image_recv):
    del y_in, gx_in
    core, at = place(sizes)
    number = functools.partial(slab_id, sizes=sizes)
    greet(core, at, -1)
    first, side, _ = sizes
    order = [(i, j, k) for k in reversed(range(side)) for j in reversed(range(side)) for i in reversed(range(first))]
    own = y_ref.shape[0] // 2
    started, loads, images = [], {}, []
    for slab in order:
        s = number(slab)
        copy = pltpu.make_async_remote_copy(
            src_ref=g_ref.at[1 - core, at(slab, 1, 1 - core)], dst_ref=swapped.at[s],
            send_sem=swap_send.at[s], recv_sem=swap_recv.at[s], device_id={"mp": 1 - core})
        copy.start()
        started.append(copy)
        loads[slab] = pltpu.make_async_copy(g_ref.at[core, at(slab)], acc.at[s], load_sem.at[s])
        loads[slab].start()
    for t, ref in enumerate((y_ref, gx_ref)):
        mine = ref.at[pl.ds(core * own, own)]
        copy = pltpu.make_async_remote_copy(
            src_ref=mine, dst_ref=mine, send_sem=image_send.at[t], recv_sem=image_recv.at[t],
            device_id={"mp": 1 - core})
        copy.start()
        started.append(copy)
        theirs = ref.at[pl.ds((1 - core) * own, own)]
        images.append(pltpu.make_async_remote_copy(
            src_ref=theirs, dst_ref=theirs, send_sem=image_send.at[t], recv_sem=image_recv.at[t],
            device_id={"mp": 1 - core}))

    def arrived(buffer, spot, sem):
        pltpu.make_async_remote_copy(
            src_ref=buffer.at[spot], dst_ref=buffer.at[spot], send_sem=swap_send.at[0], recv_sem=sem,
            device_id={"mp": 1 - core}).wait_recv()
        return buffer[spot]

    for slab in order:
        s = number(slab)
        loads[slab].wait()
        value = acc[s] + arrived(swapped, s, swap_recv.at[s])
        for r in range(3):
            if not any(slab[r + 1:]) and slab[r] + 1 < sizes[r]:
                spot = number(plus(slab, UNITS[r]))
                value = value + arrived(landed, spot - 1, recv_sem.at[spot])
        if any(slab):
            acc[s] = value
            r = max(q for q in range(3) if slab[q])
            copy = pltpu.make_async_remote_copy(
                src_ref=acc.at[s], dst_ref=landed.at[s - 1], send_sem=send_sem.at[s], recv_sem=recv_sem.at[s],
                device_id={"dp": at(UNITS[r])})
            copy.start()
            started.append(copy)
        else:
            out_ref[...] = value
    for copy in images:
        copy.wait_recv()
    for copy in started:
        copy.wait_send()


def scatter(grads, block_out, input_gradient, n):
    sizes = rings(n)
    slab = grads.shape[2:]
    anywhere = pl.BlockSpec(memory_space=pl.ANY)
    return pl.pallas_call(
        functools.partial(scatter_kernel, sizes),
        out_shape=[jax.ShapeDtypeStruct(slab, f32), jax.ShapeDtypeStruct(block_out.shape, f32),
                   jax.ShapeDtypeStruct(input_gradient.shape, f32)],
        in_specs=[anywhere] * 3,
        out_specs=[pl.BlockSpec(memory_space=pltpu.VMEM), anywhere, anywhere],
        input_output_aliases={1: 1, 2: 2},
        scratch_shapes=[
            pltpu.VMEM((n,) + slab, f32), pltpu.VMEM((n,) + slab, f32), pltpu.VMEM((n - 1,) + slab, f32),
            pltpu.SemaphoreType.DMA((n,)), pltpu.SemaphoreType.DMA((n,)), pltpu.SemaphoreType.DMA((n,)),
            pltpu.SemaphoreType.DMA((n,)), pltpu.SemaphoreType.DMA((n,)),
            pltpu.SemaphoreType.DMA((2,)), pltpu.SemaphoreType.DMA((2,)),
        ],
        compiler_params=pltpu.CompilerParams(
            collective_id=1, has_side_effects=True, vmem_limit_bytes=60 * 2**20),
        name="scatter",
    )(grads, block_out, input_gradient)


def pack_attention(mixer, output):
    head = mixer.shape[2] // 3
    pair = 2 * head
    out = output.T
    q, k, v = mixer[:, 0], mixer[:, 1], mixer[:, 2]
    return jnp.concatenate([q[:, :pair], k[:, :pair], v[:, :pair], q[:, pair:], k[:, pair:], v[:, pair:],
                            out[:, pair:], out[:, :pair]], axis=1)


def unpack_attention(block, head):
    pair = 2 * head
    cut = [block[:, t * head:(t + 1) * head] for t in range(12)]
    mixer = jnp.stack([jnp.concatenate(t, axis=1) for t in (
        (cut[0], cut[1], cut[6]), (cut[2], cut[3], cut[7]), (cut[4], cut[5], cut[8]))], axis=1)
    output = jnp.concatenate([cut[10], cut[11], cut[9]], axis=1).T
    return mixer, output


SMALL = ("first_gain", "first_shift", "output_bias", "second_gain", "second_shift", "reduce_bias",
         "mixer_bias", "expand_bias")


def pack_small(values):
    return jnp.concatenate([values[name].reshape(-1) for name in SMALL])


def unpack_small(flat, like):
    out, start = {}, 0
    for name in SMALL:
        size = like[name].size
        out[name] = flat[start:start + size].reshape(like[name].shape)
        start += size
    return out


def adam_update(param, grad, momentum, variance, decay):
    momentum_next = beta_one * momentum + (1.0 - beta_one) * grad
    variance_next = beta_two * variance + (1.0 - beta_two) * grad * grad
    mean_hat = momentum_next / (1.0 - beta_one**step_count)
    square_hat = variance_next / (1.0 - beta_two**step_count)
    stepped = param - learn_rate * (mean_hat / (jnp.sqrt(square_hat) + adam_eps) + decay * param)
    return (stepped, momentum_next, variance_next)


NAMES = ("first_gain", "first_shift", "mixer_weight", "mixer_bias", "output_weight", "output_bias", "second_gain",
         "second_shift", "expand_weight", "expand_bias", "reduce_weight", "reduce_bias")
DECAYED = ("mixer_weight", "output_weight", "expand_weight", "reduce_weight")


def per_device(inputs, cotangent, *rest):
    n = lax.axis_size("dp")
    scale = (n * inputs.shape[0] * inputs.shape[1]) ** (-0.5)
    params = dict(zip(NAMES, rest[:12]))
    momenta = dict(zip(NAMES, rest[12:24]))
    variances = dict(zip(NAMES, rest[24:]))
    share, width = params["first_gain"].shape[0], inputs.shape[2]
    heads, piece = params["mixer_bias"].shape[1:]
    head = piece * n
    hidden_local = params["expand_weight"].shape[1]
    end = 6 * LANES + 2 * hidden_local

    small = pack_small(params)
    count = small.shape[0]
    slab = jnp.concatenate([
        pack_attention(params["mixer_weight"], params["output_weight"]),
        params["expand_weight"], params["reduce_weight"].T,
        jnp.pad(small, (0, share * LANES - count)).reshape(share, LANES)], axis=1)
    columns = slab.shape[1]
    gathered = gather(slab, n)

    flat = gathered[:, :, :, end:].reshape(2, n, share * LANES)[:, :, :count]
    vectors = jnp.pad(flat[0, :, :6 * share].reshape(n, 6, share).transpose(1, 0, 2).reshape(6, width),
                      ((0, 2), (0, 0)))
    bias = flat[:, :, 6 * share:7 * share].reshape(2, n, 2, heads, piece).transpose(0, 2, 3, 1, 4)
    bias = bias.reshape(2, 2, heads * head)
    q, v, none = bias[:, 0], bias[:, 1], jnp.zeros((2, 2 * head), f32)
    mixed_bias = jnp.concatenate([q[:, :2 * head], none, v[:, :2 * head], q[:, 2 * head:], none[:, :head],
                                  v[:, 2 * head:], none[:, :head]], axis=1)[:, None]
    expand_bias = flat[:, :, 7 * share:].reshape(2, n, -1, piece).transpose(0, 2, 1, 3).reshape(2, 1, -1)

    base = (lax.axis_index("mp") * (inputs.shape[0] // 2)).astype(jnp.int32).reshape(1)
    block_out, input_gradient, grads, small_grads = run_layer(
        base, inputs, cotangent, gathered.reshape(2, width, columns), vectors, mixed_bias, expand_bias, heads, head)

    six = jnp.broadcast_to(small_grads[0, :6, :width].reshape(1, 6, n, share), (2, 6, n, share))
    six = six * (jnp.arange(2) == 0).astype(f32).reshape(2, 1, 1, 1)
    total = small_grads[:1, :6, :width].reshape(6, n, share).transpose(1, 0, 2).reshape(n, 6 * share)
    row = small_grads[:, 6, :5 * LANES]
    bias = jnp.stack([
        jnp.concatenate([row[:, :2 * head], row[:, 6 * head:7 * head]], axis=1),
        jnp.concatenate([row[:, 4 * head:6 * head], row[:, 8 * head:9 * head]], axis=1)], axis=1)
    bias = bias.reshape(2, 2, heads, n, piece).transpose(0, 3, 1, 2, 4).reshape(2, n, share)
    hidden = small_grads[:, 7].reshape(2, hidden_local // head, n, piece).transpose(0, 2, 1, 3).reshape(2, n, -1)
    packed = jnp.concatenate([jnp.broadcast_to(total[None], (2,) + total.shape), bias, hidden], axis=2)
    packed = jnp.pad(packed, ((0, 0), (0, 0), (0, share * LANES - count))).reshape(2, n, share, LANES)
    grads = lax.dynamic_update_slice(grads.reshape(2, n, share, columns), packed, (0, 0, 0, end))

    summed, block_out, input_gradient = scatter(grads, block_out, input_gradient, n)
    summed = summed * scale
    mixer, output = unpack_attention(summed[:, :6 * LANES], head)
    gradients = unpack_small(summed[:, end:].reshape(-1), params)
    gradients.update(mixer_weight=mixer, output_weight=output,
                     expand_weight=summed[:, 6 * LANES:6 * LANES + hidden_local],
                     reduce_weight=summed[:, 6 * LANES + hidden_local:end].T)
    results = [adam_update(params[m], gradients[m], momenta[m], variances[m], weight_decay if m in DECAYED else 0.0)
               for m in NAMES]
    return (block_out, input_gradient, *(gradients[m] for m in NAMES), *(r[0] for r in results),
            *(r[1] for r in results), *(r[2] for r in results))


def solution(mesh):
    images = P("dp", None, None)
    entries = (P("dp"), P("dp"), P("dp", None, "mp"), P(None, "mp", "dp"), P("mp", "dp"), P("dp"), P("dp"), P("dp"),
               P("dp", "mp"), P("mp", "dp"), P("mp", "dp"), P("dp"))
    return jax.shard_map(per_device, mesh=mesh, in_specs=(images, images) + entries * 3,
                         out_specs=(images, images) + entries * 4, check_vma=False)
```

```python
import functools
import heapq

import jax
import jax.numpy as jnp
from jax import lax
from jax.experimental import pallas as pl
from jax.experimental.pallas import tpu as pltpu
from jax.sharding import PartitionSpec as P

norm_eps = 1e-06
beta_one = 0.9
beta_two = 0.99
adam_eps = 1e-08
learn_rate = 0.05
weight_decay = 0.05
step_count = 3.0

LANES = 128
MASKED = -1e30
f32, bf16 = jnp.float32, jnp.bfloat16


def split(x):
    high = x.astype(bf16)
    return high, (x - high.astype(f32)).astype(bf16)


def dot(a, b, da, db):
    return lax.dot_general(a, b, (((da,), (db,)), ((), ())), preferred_element_type=f32)


def product(a, b, da, db):
    left = jnp.concatenate([a[0], a[0], a[1]], axis=da)
    right = jnp.concatenate([b[0], b[1], b[0]], axis=db)
    return dot(left, right, da, db)


def product_apart(a, b, da, db):
    return dot(a[0], b[0], da, db) + dot(a[0], b[1], da, db) + dot(a[1], b[0], da, db)


def layer_kernel(length, heads, head, base, x_ref, cot_ref, w_ref, vec_ref, mb_ref, eb_ref,
                 y_ref, gx_ref, g_ref, sg_ref,
                 whi, wlo, wsem, pad, mixed, probs_hi, probs_lo, joined,
                 fo_hi, fo_lo, so_hi, so_lo, cot_hi, cot_lo, gm_hi, gm_lo, part, part2):
    step = pl.program_id(0)
    rows, width = pad.shape[1], pad.shape[2]
    local = heads * head
    qkv = 5 * LANES
    hidden_local = eb_ref.shape[-1]
    attn = 6 * LANES
    up, down, end = attn, attn + hidden_local, attn + 2 * hidden_local

    @pl.when(step == 0)
    def _():
        for c in range(2):
            pltpu.make_async_copy(w_ref.at[c], g_ref.at[c], wsem.at[c]).start()
        pad[...] = jnp.zeros_like(pad)
        sg_ref[...] = jnp.zeros_like(sg_ref)
        for c in range(2):
            pltpu.make_async_copy(w_ref.at[c], g_ref.at[c], wsem.at[c]).wait()

        def convert(t, _):
            c, r = t // (width // 16), t % (width // 16)
            at = pl.ds(pl.multiple_of(r * 16, 16), 16)
            high, low = split(g_ref[c, at, 0:end])
            whi[c, at, :] = high
            wlo[c, at, :] = low
            g_ref[c, at, :] = jnp.zeros((16, g_ref.shape[2]), f32)
            return 0

        lax.fori_loop(0, 2 * (width // 16), convert, 0)

    def weight(c, lo, hi):
        return whi[c, :, lo:hi], wlo[c, :, lo:hi]

    def vec(r):
        return vec_ref[r:r + 1, :]

    def normalize(v):
        center = v - jnp.mean(v, axis=-1, keepdims=True)
        inverse = lax.rsqrt(jnp.mean(center * center, axis=-1, keepdims=True) + norm_eps)
        return center * inverse, inverse

    def norm_back(grad, normed, inverse, gain):
        scaled = grad * gain
        return inverse * (scaled - jnp.mean(scaled, axis=-1, keepdims=True)
                          - normed * jnp.mean(scaled * normed, axis=-1, keepdims=True))

    def total(v):
        return jnp.sum(v, axis=0, keepdims=True)

    pad[0, 0:length, :] = x_ref[0]
    pad[1, 0:length, :] = cot_ref[0]
    x, cot = pad[0], pad[1]
    cot_hi[...], cot_lo[...] = split(cot)
    first, first_inverse = normalize(x)
    fo_hi[...], fo_lo[...] = split(first * vec(0) + vec(1))

    lane = lax.broadcasted_iota(jnp.int32, (rows, LANES), 1)
    sides = (lane < head, lane >= head)
    column = lax.broadcasted_iota(jnp.int32, (rows, rows), 1)
    score_scale = head ** (-0.5)

    def side(v, s):
        return jnp.where(sides[s], v, 0.0)

    def swap(v):
        return pltpu.roll(v, head, 1)

    def windows(c):
        w = [mixed[c, :, t * LANES:(t + 1) * LANES] for t in range(5)]
        third = side(w[3], 0) * score_scale, side(swap(w[3]), 0), side(w[4], 0)
        return [
            (side(w[0], 0) * score_scale, side(w[1], 0), side(w[2], 0)),
            (side(w[0], 1) * score_scale, side(w[1], 1), side(w[2], 1)),
            third,
        ]

    part[...] = jnp.zeros_like(part)

    def attend(c, _):
        mixed[c] = product((fo_hi[...], fo_lo[...]), weight(c, 0, qkv), 1, 0) + mb_ref[c]
        outs = []
        for h, (q, k, v) in enumerate(windows(c)):
            scores = product(split(q), split(k), 1, 1)
            scores = jnp.where(column < length, scores, MASKED)
            expon = jnp.exp(scores - jnp.max(scores, axis=-1, keepdims=True))
            probs = split(expon / jnp.sum(expon, axis=-1, keepdims=True))
            probs_hi[c, h], probs_lo[c, h] = probs
            outs.append(product_apart(probs, split(v), 1, 0))
        joined[c] = jnp.concatenate([swap(outs[2]), outs[0] + outs[1]], axis=1)
        part[...] += product(split(joined[c]), weight(c, 4 * LANES, attn), 1, 1)
        return 0

    lax.fori_loop(0, 2, attend, 0)
    middle = x + part[...] + vec(2)
    second, second_inverse = normalize(middle)
    so_hi[...], so_lo[...] = split(second * vec(3) + vec(4))

    part[...] = middle + vec(5)
    part2[...] = jnp.zeros_like(part2)

    def feed(c, _):
        so = (so_hi[...], so_lo[...])
        co = (cot_hi[...], cot_lo[...])
        hidden = product(so, weight(c, up, down), 1, 0) + eb_ref[c]
        share = 0.5 * (1.0 + lax.erf(hidden * (0.5 ** 0.5)))
        active = split(hidden * share)
        slope = share + hidden * jnp.exp(-0.5 * hidden * hidden) * 0.3989422804014327
        part[...] += product(active, weight(c, down, end), 1, 1)
        g_ref[c, :, down:end] += product(co, active, 0, 0)
        grad = product(co, weight(c, down, end), 1, 0) * slope
        sg_ref[c, 7:8, 0:hidden_local] += total(grad)
        grad = split(grad)
        g_ref[c, :, up:down] += product(so, grad, 0, 0)
        part2[...] += product(grad, weight(c, up, down), 1, 1)
        return 0

    lax.fori_loop(0, 2, feed, 0)
    y_ref[0] = part[0:length, :]

    grad_second = part2[...]
    sg_ref[0, 3:4, 0:width] += total(grad_second * second)
    sg_ref[0, 4:5, 0:width] += total(grad_second)
    sg_ref[0, 5:6, 0:width] += total(cot)
    grad_middle = cot + norm_back(grad_second, second, second_inverse, vec(3))
    sg_ref[0, 2:3, 0:width] += total(grad_middle)
    gm_hi[...], gm_lo[...] = split(grad_middle)
    part2[...] = grad_middle

    part[...] = jnp.zeros_like(part)

    def attend_back(c, _):
        gm = (gm_hi[...], gm_lo[...])
        fo = (fo_hi[...], fo_lo[...])
        grad_heads = product(gm, weight(c, 4 * LANES, attn), 1, 0)
        g_ref[c, :, 4 * LANES:attn] += product(gm, split(joined[c]), 0, 0)
        pair, single = grad_heads[:, LANES:], swap(grad_heads[:, :LANES])
        pair_out, single_out = joined[c, :, LANES:], swap(joined[c, :, :LANES])
        grad_outs = (side(pair, 0), side(pair, 1), side(single, 0))
        outs = (pair_out, pair_out, single_out)
        grads = []
        for h, (q, k, v) in enumerate(windows(c)):
            grad_out = grad_outs[h]
            row = jnp.sum(grad_out * outs[h], axis=-1, keepdims=True)
            grad_out = split(grad_out)
            grad_probs = product(grad_out, split(v), 1, 1)
            probs = (probs_hi[c, h], probs_lo[c, h])
            grad_v = product(probs, grad_out, 0, 0)
            grad_scores = split((probs[0].astype(f32) + probs[1].astype(f32)) * (grad_probs - row))
            grad_q = product_apart(grad_scores, split(k), 1, 0) * score_scale
            grad_k = product(grad_scores, split(q), 0, 0)
            grads.append((grad_q, grad_k, grad_v))
        one, two, three = grads
        grad_mixed = jnp.concatenate(
            [one[0] + two[0], one[1] + two[1], one[2] + two[2], three[0] + swap(three[1]), three[2]], axis=1)
        sg_ref[c, 6:7, 0:qkv] += total(grad_mixed)
        grad_mixed = split(grad_mixed)
        g_ref[c, :, 0:qkv] += product(fo, grad_mixed, 0, 0)
        part[...] += product(grad_mixed, weight(c, 0, qkv), 1, 1)
        return 0

    lax.fori_loop(0, 2, attend_back, 0)
    grad_first = part[...]
    sg_ref[0, 0:1, 0:width] += total(grad_first * first)
    sg_ref[0, 1:2, 0:width] += total(grad_first)
    gx_ref[0] = (part2[...] + norm_back(grad_first, first, first_inverse, vec(0)))[0:length, :]


def run_layer(base, inputs, cotangent, weights, vectors, mixed_bias, expand_bias, heads, head):
    images, length, width = inputs.shape
    own = images // 2
    rows = -(-length // 16) * 16
    columns = weights.shape[-1]
    hidden_local = expand_bias.shape[-1]
    end = 6 * LANES + 2 * hidden_local
    image = pl.BlockSpec((1, length, width), lambda i, b: (b[0] + i, 0, 0))

    def whole(shape):
        return pl.BlockSpec(shape, lambda i, b: (0,) * len(shape))

    act = pltpu.VMEM((rows, width), bf16)
    return pl.pallas_call(
        functools.partial(layer_kernel, length, heads, head),
        grid_spec=pltpu.PrefetchScalarGridSpec(
            num_scalar_prefetch=1,
            grid=(own,),
            in_specs=[image, image, pl.BlockSpec(memory_space=pl.ANY), whole(vectors.shape),
                      whole(mixed_bias.shape), whole(expand_bias.shape)],
            out_specs=[image, image, whole((2, width, columns)), whole((2, 8, hidden_local))],
            scratch_shapes=[
                pltpu.VMEM((2, width, end), bf16), pltpu.VMEM((2, width, end), bf16),
                pltpu.SemaphoreType.DMA((2,)),
                pltpu.VMEM((2, rows, width), f32),
                pltpu.VMEM((2, rows, 5 * LANES), f32),
                pltpu.VMEM((2, heads, rows, rows), bf16), pltpu.VMEM((2, heads, rows, rows), bf16),
                pltpu.VMEM((2, rows, 2 * LANES), f32),
                act, act, act, act, act, act, act, act,
                pltpu.VMEM((rows, width), f32), pltpu.VMEM((rows, width), f32),
            ],
        ),
        out_shape=[
            jax.ShapeDtypeStruct(inputs.shape, f32), jax.ShapeDtypeStruct(inputs.shape, f32),
            jax.ShapeDtypeStruct((2, width, columns), f32), jax.ShapeDtypeStruct((2, 8, hidden_local), f32),
        ],
        compiler_params=pltpu.CompilerParams(
            dimension_semantics=("arbitrary",), vmem_limit_bytes=60 * 2**20),
        name="layer",
    )(base, inputs, cotangent, weights, vectors, mixed_bias, expand_bias)


def rings(n):
    side = max(k for k in range(1, n + 1) if n % (k * k) == 0 and n // (k * k) >= k)
    return n // (side * side), side, side


def place(sizes):
    first, side, _ = sizes
    core, me = lax.axis_index("mp"), lax.axis_index("dp")
    a, b, c = me // (side * side), (me // side) % side, me % side

    def at(slab, sign=1, of=core):
        i, j, k = slab
        i, j, k = (sign * i) % first, (sign * j) % side, (sign * k) % side
        ahead_b = j * of + k * (1 - of)
        ahead_c = k * of + j * (1 - of)
        return (((a + i) % first) * side + (b + ahead_b) % side) * side + (c + ahead_c) % side

    return core, at


UNITS = ((1, 0, 0), (0, 1, 0), (0, 0, 1))


def plus(slab, unit):
    return tuple(s + u for s, u in zip(slab, unit))


def sends(slab, sizes):
    return [r for r in range(3) if not any(slab[r + 1:]) and slab[r] + 1 < sizes[r]]


def arrival_order(sizes):
    cost, free, heap, order = (2.0, 1.5, 1.5), [0.0] * 3, [(0.0, (0, 0, 0))], []
    while heap:
        now, slab = heapq.heappop(heap)
        order.append(slab)
        for r in sends(slab, sizes):
            free[r] = max(now, free[r]) + cost[r]
            heapq.heappush(heap, (free[r], plus(slab, UNITS[r])))
    return order


def slab_id(slab, sizes):
    return (slab[0] * sizes[1] + slab[1]) * sizes[2] + slab[2]


def greet(core, at, sign):
    barrier = pltpu.get_barrier_semaphore()
    for unit in UNITS:
        pl.semaphore_signal(barrier, inc=1, device_id={"dp": at(unit, sign)})
    pl.semaphore_signal(barrier, inc=1, device_id={"mp": 1 - core})
    pl.semaphore_wait(barrier, 4)


def gather_kernel(sizes, slab_ref, out_ref, send_sem, recv_sem, swap_send, swap_recv, own_sem):
    core, at = place(sizes)
    number = functools.partial(slab_id, sizes=sizes)
    greet(core, at, -1)

    def landing(slab, of):
        return out_ref.at[of, at(slab, -1, of)]

    started = []
    own = pltpu.make_async_copy(slab_ref, landing((0, 0, 0), core), own_sem)
    for slab in arrival_order(sizes):
        spot = landing(slab, core)
        if any(slab):
            pltpu.make_async_remote_copy(
                src_ref=spot, dst_ref=spot, send_sem=send_sem.at[0, 0], recv_sem=recv_sem.at[number(slab)],
                device_id={"mp": 1 - core}).wait_recv()
        source = spot if any(slab) else slab_ref
        for r in reversed(sends(slab, sizes)):
            copy = pltpu.make_async_remote_copy(
                src_ref=source, dst_ref=spot, send_sem=send_sem.at[r, number(slab)],
                recv_sem=recv_sem.at[number(plus(slab, UNITS[r]))], device_id={"dp": at(UNITS[r])})
            copy.start()
            started.append(copy)
        copy = pltpu.make_async_remote_copy(
            src_ref=source, dst_ref=spot, send_sem=swap_send.at[number(slab)], recv_sem=swap_recv.at[number(slab)],
            device_id={"mp": 1 - core})
        copy.start()
        started.append(copy)
        if not any(slab):
            own.start()
    for slab in arrival_order(sizes):
        spot = landing(slab, 1 - core)
        pltpu.make_async_remote_copy(
            src_ref=spot, dst_ref=spot, send_sem=swap_send.at[0], recv_sem=swap_recv.at[number(slab)],
            device_id={"mp": 1 - core}).wait_recv()
    for copy in started:
        copy.wait_send()
    own.wait()


def gather(slab, n):
    sizes = rings(n)
    return pl.pallas_call(
        functools.partial(gather_kernel, sizes),
        out_shape=jax.ShapeDtypeStruct((2, n) + slab.shape, f32),
        in_specs=[pl.BlockSpec(memory_space=pltpu.VMEM)],
        out_specs=pl.BlockSpec(memory_space=pl.ANY),
        scratch_shapes=[
            pltpu.SemaphoreType.DMA((3, n)), pltpu.SemaphoreType.DMA((n,)),
            pltpu.SemaphoreType.DMA((n,)), pltpu.SemaphoreType.DMA((n,)), pltpu.SemaphoreType.DMA,
        ],
        compiler_params=pltpu.CompilerParams(collective_id=0, has_side_effects=True),
        name="gather",
    )(slab)


def scatter_kernel(sizes, g_ref, y_in, gx_in, out_ref, y_ref, gx_ref,
                   acc, swapped, landed, load_sem, send_sem, recv_sem, swap_send, swap_recv, image_send, image_recv):
    del y_in, gx_in
    core, at = place(sizes)
    number = functools.partial(slab_id, sizes=sizes)
    greet(core, at, -1)
    first, side, _ = sizes
    order = [(i, j, k) for k in reversed(range(side)) for j in reversed(range(side)) for i in reversed(range(first))]
    own = y_ref.shape[0] // 2
    started, loads, images = [], {}, []
    for slab in order:
        s = number(slab)
        copy = pltpu.make_async_remote_copy(
            src_ref=g_ref.at[1 - core, at(slab, 1, 1 - core)], dst_ref=swapped.at[s],
            send_sem=swap_send.at[s], recv_sem=swap_recv.at[s], device_id={"mp": 1 - core})
        copy.start()
        started.append(copy)
        loads[slab] = pltpu.make_async_copy(g_ref.at[core, at(slab)], acc.at[s], load_sem.at[s])
        loads[slab].start()
    for t, ref in enumerate((y_ref, gx_ref)):
        mine = ref.at[pl.ds(core * own, own)]
        copy = pltpu.make_async_remote_copy(
            src_ref=mine, dst_ref=mine, send_sem=image_send.at[t], recv_sem=image_recv.at[t],
            device_id={"mp": 1 - core})
        copy.start()
        started.append(copy)
        theirs = ref.at[pl.ds((1 - core) * own, own)]
        images.append(pltpu.make_async_remote_copy(
            src_ref=theirs, dst_ref=theirs, send_sem=image_send.at[t], recv_sem=image_recv.at[t],
            device_id={"mp": 1 - core}))

    def arrived(buffer, spot, sem):
        pltpu.make_async_remote_copy(
            src_ref=buffer.at[spot], dst_ref=buffer.at[spot], send_sem=swap_send.at[0], recv_sem=sem,
            device_id={"mp": 1 - core}).wait_recv()
        return buffer[spot]

    for slab in order:
        s = number(slab)
        loads[slab].wait()
        value = acc[s] + arrived(swapped, s, swap_recv.at[s])
        for r in range(3):
            if not any(slab[r + 1:]) and slab[r] + 1 < sizes[r]:
                spot = number(plus(slab, UNITS[r]))
                value = value + arrived(landed, spot - 1, recv_sem.at[spot])
        if any(slab):
            acc[s] = value
            r = max(q for q in range(3) if slab[q])
            copy = pltpu.make_async_remote_copy(
                src_ref=acc.at[s], dst_ref=landed.at[s - 1], send_sem=send_sem.at[s], recv_sem=recv_sem.at[s],
                device_id={"dp": at(UNITS[r])})
            copy.start()
            started.append(copy)
        else:
            out_ref[...] = value
    for copy in images:
        copy.wait_recv()
    for copy in started:
        copy.wait_send()


def scatter(grads, block_out, input_gradient, n):
    sizes = rings(n)
    slab = grads.shape[2:]
    anywhere = pl.BlockSpec(memory_space=pl.ANY)
    return pl.pallas_call(
        functools.partial(scatter_kernel, sizes),
        out_shape=[jax.ShapeDtypeStruct(slab, f32), jax.ShapeDtypeStruct(block_out.shape, f32),
                   jax.ShapeDtypeStruct(input_gradient.shape, f32)],
        in_specs=[anywhere] * 3,
        out_specs=[pl.BlockSpec(memory_space=pltpu.VMEM), anywhere, anywhere],
        input_output_aliases={1: 1, 2: 2},
        scratch_shapes=[
            pltpu.VMEM((n,) + slab, f32), pltpu.VMEM((n,) + slab, f32), pltpu.VMEM((n - 1,) + slab, f32),
            pltpu.SemaphoreType.DMA((n,)), pltpu.SemaphoreType.DMA((n,)), pltpu.SemaphoreType.DMA((n,)),
            pltpu.SemaphoreType.DMA((n,)), pltpu.SemaphoreType.DMA((n,)),
            pltpu.SemaphoreType.DMA((2,)), pltpu.SemaphoreType.DMA((2,)),
        ],
        compiler_params=pltpu.CompilerParams(
            collective_id=1, has_side_effects=True, vmem_limit_bytes=60 * 2**20),
        name="scatter",
    )(grads, block_out, input_gradient)


def spread(count, slots, lead):
    return [min(slots - 1, lead + (e * (slots - lead)) // count) for e in range(count)]


def step_kernel(sizes, length, heads, head, slab_ref, x_ref, cot_ref, out_ref, y_ref, gx_ref,
                buf, whi, wlo, xs, cots, fo_hi, fo_lo, so_hi, so_lo, cot_hi, cot_lo, gm_hi, gm_lo,
                mixed, probs_hi, probs_lo, joined, mid, back, yb, staged, vec_ref, bias_ref, hidden_bias, small_grads,
                swapped, landed, send_sem, recv_sem, swap_send, swap_recv,
                push_send, push_recv, trade_send, trade_recv, stage_sem, image_sem, image_send, image_recv):
    core, at = place(sizes)
    number = functools.partial(slab_id, sizes=sizes)
    n = sizes[0] * sizes[1] * sizes[2]
    own, rows, width = xs.shape
    share = slab_ref.shape[0]
    hidden_local = hidden_bias.shape[-1]
    qkv, attn = 5 * LANES, 6 * LANES
    small, up = attn, attn + LANES
    down, end = up + hidden_local, up + 2 * hidden_local
    spans = ((0, up), (up, end))
    partner = {"mp": 1 - core}

    def block(slab, sign, of):
        return pl.ds(pl.multiple_of(at(slab, sign, of) * share, 8), share)

    def span(p):
        return slice(*spans[p])

    def landing(p, slab, of):
        return buf.at[of, block(slab, -1, of), span(p)]

    def gather_event(p, slab):
        spot = landing(p, slab, core)
        if any(slab):
            pltpu.make_async_remote_copy(
                src_ref=spot, dst_ref=spot, send_sem=send_sem.at[p, 0, 0], recv_sem=recv_sem.at[p, number(slab)],
                device_id=partner).wait_recv()
        source = spot if any(slab) else slab_ref.at[:, span(p)]
        for r in reversed(sends(slab, sizes)):
            pltpu.make_async_remote_copy(
                src_ref=source, dst_ref=spot, send_sem=send_sem.at[p, r, number(slab)],
                recv_sem=recv_sem.at[p, number(plus(slab, UNITS[r]))], device_id={"dp": at(UNITS[r])}).start()
        pltpu.make_async_remote_copy(
            src_ref=source, dst_ref=spot, send_sem=swap_send.at[p, number(slab)],
            recv_sem=swap_recv.at[p, number(slab)], device_id=partner).start()

    def gather_end(p):
        for slab in order:
            spot = landing(p, slab, 1 - core)
            pltpu.make_async_remote_copy(
                src_ref=spot, dst_ref=spot, send_sem=swap_send.at[p, 0], recv_sem=swap_recv.at[p, number(slab)],
                device_id=partner).wait_recv()
        for slab in order:
            spot = landing(p, slab, core)
            for r in sends(slab, sizes):
                pltpu.make_async_remote_copy(
                    src_ref=spot, dst_ref=spot, send_sem=send_sem.at[p, r, number(slab)],
                    recv_sem=recv_sem.at[p, 0], device_id=partner).wait_send()
            pltpu.make_async_remote_copy(
                src_ref=spot, dst_ref=spot, send_sem=swap_send.at[p, number(slab)], recv_sem=swap_recv.at[p, 0],
                device_id=partner).wait_send()

    order = arrival_order(sizes)

    first_size, side_size, _ = sizes
    back_order = [(i, j, k) for k in reversed(range(side_size)) for j in reversed(range(side_size))
                  for i in reversed(range(first_size))]

    def trade(p, slab):
        s = number(slab)
        return pltpu.make_async_remote_copy(
            src_ref=buf.at[1 - core, block(slab, 1, 1 - core), span(p)], dst_ref=swapped.at[s, :, span(p)],
            send_sem=trade_send.at[p, s], recv_sem=trade_recv.at[p, s], device_id=partner)

    def scatter_start(p):
        for slab in back_order:
            trade(p, slab).start()

    def arrived(buffer, spot, p, sem):
        ref = buffer.at[spot, :, span(p)]
        pltpu.make_async_remote_copy(
            src_ref=ref, dst_ref=ref, send_sem=trade_send.at[p, 0], recv_sem=sem, device_id=partner).wait_recv()
        return ref[...]

    def push(p, slab):
        s = number(slab)
        r = max(q for q in range(3) if slab[q])
        return pltpu.make_async_remote_copy(
            src_ref=buf.at[core, block(slab, 1, core), span(p)], dst_ref=landed.at[s - 1, :, span(p)],
            send_sem=push_send.at[p, s], recv_sem=push_recv.at[p, s], device_id={"dp": at(UNITS[r])})

    def scatter_event(p, slab):
        s = number(slab)
        here = (core, block(slab, 1, core), span(p))
        value = buf[here] + arrived(swapped, s, p, trade_recv.at[p, s])
        for r in range(3):
            if not any(slab[r + 1:]) and slab[r] + 1 < sizes[r]:
                spot = number(plus(slab, UNITS[r]))
                value = value + arrived(landed, spot - 1, p, push_recv.at[p, spot])
        if any(slab):
            buf[here] = value
            push(p, slab).start()
        else:
            out_ref[:, span(p)] = value

    def scatter_end(p):
        for slab in back_order:
            trade(p, slab).wait_send()
            if any(slab):
                push(p, slab).wait_send()

    def image_copies(t, source, ref, i):
        spot = ref.at[core * own + i]
        keep = pltpu.make_async_copy(source.at[i], spot, image_sem.at[t, i])
        give = pltpu.make_async_remote_copy(
            src_ref=source.at[i], dst_ref=spot, send_sem=image_send.at[t, i], recv_sem=image_recv.at[t, i],
            device_id=partner)
        theirs = ref.at[(1 - core) * own + i]
        take = pltpu.make_async_remote_copy(
            src_ref=theirs, dst_ref=theirs, send_sem=image_send.at[t, i], recv_sem=image_recv.at[t, i],
            device_id=partner)
        return keep, give, take

    def weight(c, lo, hi):
        return whi[c, :, lo:hi], wlo[c, :, lo:hi]

    def vec(r):
        return vec_ref[r:r + 1, :]

    def normalize(v):
        center = v - jnp.mean(v, axis=-1, keepdims=True)
        inverse = lax.rsqrt(jnp.mean(center * center, axis=-1, keepdims=True) + norm_eps)
        return center * inverse, inverse

    def norm_back(grad, normed, inverse, gain):
        scaled = grad * gain
        return inverse * (scaled - jnp.mean(scaled, axis=-1, keepdims=True)
                          - normed * jnp.mean(scaled * normed, axis=-1, keepdims=True))

    def total(v):
        return jnp.sum(v, axis=0, keepdims=True)

    def convert(lo, hi):
        def body(t, _):
            c, r = t // (width // 16), t % (width // 16)
            here = pl.ds(pl.multiple_of(r * 16, 16), 16)
            high, low = split(buf[c, here, lo:hi])
            whi[c, here, lo:hi] = high
            wlo[c, here, lo:hi] = low
            buf[c, here, lo:hi] = jnp.zeros((16, hi - lo), f32)
            return 0

        lax.fori_loop(0, 2 * (width // 16), body, 0)

    def thirds(v):
        high = v.astype(bf16)
        v = v - high.astype(f32)
        middle_term = v.astype(bf16)
        return high, middle_term, (v - middle_term.astype(f32)).astype(bf16)

    def moved(v, onehot, dim):
        return sum(dot(term, onehot, 1, dim) for term in reversed(thirds(v)))

    piece = head // n
    entry = lax.broadcasted_iota(jnp.int32, (width, LANES), 0)
    owner, inner = entry // share, entry % share
    target = lax.broadcasted_iota(jnp.int32, (width, LANES), 1)

    def attention_bias_at(t):
        kind, which = inner // (heads * piece), (inner // piece) % heads
        window = jnp.where(kind == 0, jnp.where(which < 2, 0, 3), jnp.where(which < 2, 2, 4))
        place_in = (which % 2) * head + owner * piece + inner % piece
        return ((window == t) & (place_in == target)).astype(f32).astype(bf16)

    def hidden_bias_at(half, t):
        flat = inner + half * share
        place_in = (flat // piece) * head + owner * piece + flat % piece
        return (place_in == target + t * LANES).astype(f32).astype(bf16)

    greet(core, at, -1)
    gather_event(0, (0, 0, 0))
    staging = []
    tiles = width // LANES
    for t in range(tiles):
        staging.append(pltpu.make_async_copy(x_ref.at[:, t * LANES:(t + 1) * LANES], staged.at[t], stage_sem.at[t]))
        staging[-1].start()
    buf[core, block((0, 0, 0), 1, core), :] = slab_ref[...]
    xs[...] = jnp.zeros_like(xs)
    cots[...] = jnp.zeros_like(cots)
    small_grads[...] = jnp.zeros_like(small_grads)
    for source, sink in ((x_ref, xs), (cot_ref, cots)):
        for t in range(tiles):
            lanes = slice(t * LANES, (t + 1) * LANES)
            copy = pltpu.make_async_copy(source.at[:, lanes], staged.at[t], stage_sem.at[t])
            if sink is cots:
                copy.start()
            copy.wait()
            for i in range(own):
                sink[i, 0:length, lanes] = staged[t, pl.ds(core * own + i, length, stride=2 * own), :]

    for slab in order[1:]:
        gather_event(0, slab)
    gather_event(1, (0, 0, 0))
    for i in range(own):
        cot_hi[i], cot_lo[i] = split(cots[i])
    gather_end(0)
    for c in range(2):
        turned = buf[c, :, small:up].T
        if c == 0:
            vec_ref[...] = turned[0:8, :]
        packed = turned[0:16, :]
        for t in range(5):
            bias_ref[c, :, t * LANES:(t + 1) * LANES] = moved(packed[6:7], attention_bias_at(t), 0)
        for t in range(hidden_local // LANES):
            hidden_bias[c, :, t * LANES:(t + 1) * LANES] = (
                moved(packed[7:8], hidden_bias_at(0, t), 0) + moved(packed[8:9], hidden_bias_at(1, t), 0))
    convert(0, attn)

    lane = lax.broadcasted_iota(jnp.int32, (rows, LANES), 1)
    sides = (lane < head, lane >= head)
    column = lax.broadcasted_iota(jnp.int32, (rows, rows), 1)
    score_scale = head ** (-0.5)

    def side(v, s):
        return jnp.where(sides[s], v, 0.0)

    def swap(v):
        return pltpu.roll(v, head, 1)

    def windows(i, c):
        w = [mixed[i, c, :, t * LANES:(t + 1) * LANES] for t in range(5)]
        return [
            (side(w[0], 0) * score_scale, side(w[1], 0), side(w[2], 0)),
            (side(w[0], 1) * score_scale, side(w[1], 1), side(w[2], 1)),
            (side(w[3], 0) * score_scale, side(swap(w[3]), 0), side(w[4], 0)),
        ]

    def serve(t, h, plan, event):
        for slot, slab in plan:
            if slot % heads == h:
                pl.when(t == slot // heads)(functools.partial(event, 1, slab))

    gather_plan = list(zip(spread(len(order) - 1, 2 * own * heads, 1), order[1:]))

    def attend(t, _):
        i, c = t // 2, t % 2

        @pl.when(c == 0)
        def _():
            normed, _ = normalize(xs[i])
            fo_hi[i], fo_lo[i] = split(normed * vec(0) + vec(1))
            mid[i] = xs[i] + vec(2)

        mixed[i, c] = product((fo_hi[i], fo_lo[i]), weight(c, 0, qkv), 1, 0) + bias_ref[c]
        outs = []
        for h, (q, k, v) in enumerate(windows(i, c)):
            serve(t, h, gather_plan, gather_event)
            scores = product(split(q), split(k), 1, 1)
            scores = jnp.where(column < length, scores, MASKED)
            expon = jnp.exp(scores - jnp.max(scores, axis=-1, keepdims=True))
            probs = split(expon / jnp.sum(expon, axis=-1, keepdims=True))
            probs_hi[i, c, h], probs_lo[i, c, h] = probs
            outs.append(product_apart(probs, split(v), 1, 0))
        joined[i, c] = jnp.concatenate([swap(outs[2]), outs[0] + outs[1]], axis=1)
        mid[i] += product(split(joined[i, c]), weight(c, 4 * LANES, attn), 1, 1)
        return 0

    lax.fori_loop(0, 2 * own, attend, 0)
    gather_end(1)
    convert(up, end)

    def feed(t, _):
        i, c = t // 2, t % 2

        @pl.when(c == 0)
        def _():
            second, _ = normalize(mid[i])
            so_hi[i], so_lo[i] = split(second * vec(3) + vec(4))
            yb[i] = mid[i] + vec(5)
            back[i] = jnp.zeros((rows, width), f32)

        so = (so_hi[i], so_lo[i])
        co = (cot_hi[i], cot_lo[i])
        hidden = product(so, weight(c, up, down), 1, 0) + hidden_bias[c]
        portion = 0.5 * (1.0 + lax.erf(hidden * (0.5 ** 0.5)))
        active = split(hidden * portion)
        slope = portion + hidden * jnp.exp(-0.5 * hidden * hidden) * 0.3989422804014327
        yb[i] += product(active, weight(c, down, end), 1, 1)
        buf[c, :, down:end] += product(co, active, 0, 0)
        grad = product(co, weight(c, down, end), 1, 0) * slope
        small_grads[c, 7:8, 0:hidden_local] += total(grad)
        grad = split(grad)
        buf[c, :, up:down] += product(so, grad, 0, 0)
        back[i] += product(grad, weight(c, up, down), 1, 1)

        @pl.when(c == 1)
        def _():
            cot = cots[i]
            second, second_inverse = normalize(mid[i])
            grad_second = back[i]
            small_grads[0, 3:4, 0:width] += total(grad_second * second)
            small_grads[0, 4:5, 0:width] += total(grad_second)
            small_grads[0, 5:6, 0:width] += total(cot)
            grad_middle = cot + norm_back(grad_second, second, second_inverse, vec(3))
            small_grads[0, 2:3, 0:width] += total(grad_middle)
            gm_hi[i], gm_lo[i] = split(grad_middle)
            back[i] = grad_middle
            mid[i] = jnp.zeros((rows, width), f32)

        return 0

    lax.fori_loop(0, 2 * own, feed, 0)

    scatter_start(1)
    for i in range(own):
        keep, give, _ = image_copies(0, yb, y_ref, i)
        keep.start()
        give.start()
    scatter_plan = list(zip(spread(len(back_order), 2 * own * heads, 1), back_order))

    def attend_back(t, _):
        i, c = t // 2, t % 2
        gm = (gm_hi[i], gm_lo[i])
        fo = (fo_hi[i], fo_lo[i])
        grad_heads = product(gm, weight(c, 4 * LANES, attn), 1, 0)
        buf[c, :, 4 * LANES:attn] += product(gm, split(joined[i, c]), 0, 0)
        pair, single = grad_heads[:, LANES:], swap(grad_heads[:, :LANES])
        pair_out, single_out = joined[i, c, :, LANES:], swap(joined[i, c, :, :LANES])
        grad_outs = (side(pair, 0), side(pair, 1), side(single, 0))
        outs = (pair_out, pair_out, single_out)
        grads = []
        for h, (q, k, v) in enumerate(windows(i, c)):
            serve(t, h, scatter_plan, scatter_event)
            grad_out = grad_outs[h]
            row = jnp.sum(grad_out * outs[h], axis=-1, keepdims=True)
            grad_out = split(grad_out)
            grad_probs = product(grad_out, split(v), 1, 1)
            probs = (probs_hi[i, c, h], probs_lo[i, c, h])
            grad_v = product(probs, grad_out, 0, 0)
            grad_scores = split((probs[0].astype(f32) + probs[1].astype(f32)) * (grad_probs - row))
            grad_q = product_apart(grad_scores, split(k), 1, 0) * score_scale
            grad_k = product(grad_scores, split(q), 0, 0)
            grads.append((grad_q, grad_k, grad_v))
        one, two, three = grads
        grad_mixed = jnp.concatenate(
            [one[0] + two[0], one[1] + two[1], one[2] + two[2], three[0] + swap(three[1]), three[2]], axis=1)
        small_grads[c, 6:7, 0:qkv] += total(grad_mixed)
        grad_mixed = split(grad_mixed)
        buf[c, :, 0:qkv] += product(fo, grad_mixed, 0, 0)
        mid[i] += product(grad_mixed, weight(c, 0, qkv), 1, 1)

        @pl.when(c == 1)
        def _():
            first, first_inverse = normalize(xs[i])
            grad_first = mid[i]
            small_grads[0, 0:1, 0:width] += total(grad_first * first)
            small_grads[0, 1:2, 0:width] += total(grad_first)
            xs[i] = back[i] + norm_back(grad_first, first, first_inverse, vec(0))

        return 0

    lax.fori_loop(0, 2 * own, attend_back, 0)

    for c in range(2):
        bias = sum(moved(small_grads[c, 6:7, t * LANES:(t + 1) * LANES], attention_bias_at(t), 1) for t in range(5))
        hidden = [sum(moved(small_grads[c, 7:8, t * LANES:(t + 1) * LANES], hidden_bias_at(half, t), 1)
                      for t in range(hidden_local // LANES)) for half in range(2)]
        six = small_grads[0, 0:6, 0:width]
        packed = jnp.concatenate([six, bias, hidden[0], hidden[1], jnp.zeros((LANES - 9, width), f32)], axis=0)
        buf[c, :, small:up] = packed.T
    scatter_start(0)
    for i in range(own):
        keep, give, _ = image_copies(1, xs, gx_ref, i)
        keep.start()
        give.start()
    for slab in back_order:
        scatter_event(0, slab)
    for t, source, ref in ((0, yb, y_ref), (1, xs, gx_ref)):
        for i in range(own):
            keep, give, take = image_copies(t, source, ref, i)
            keep.wait()
            give.wait_send()
            take.wait_recv()
    scatter_end(1)
    scatter_end(0)


def run_step(slab, inputs, cotangent, n, heads, head, length):
    sizes = rings(n)
    width = inputs.shape[1]
    images = inputs.shape[0] // length
    own = images // 2
    rows = -(-length // 16) * 16
    share, columns = slab.shape
    hidden_local = (columns - 7 * LANES) // 2
    anywhere = pl.BlockSpec(memory_space=pl.ANY)
    act = pltpu.VMEM((own, rows, width), bf16)
    full = pltpu.VMEM((own, rows, width), f32)
    dma = pltpu.SemaphoreType.DMA
    probs = pltpu.VMEM((own, 2, heads, rows, rows), bf16)
    return pl.pallas_call(
        functools.partial(step_kernel, sizes, length, heads, head),
        out_shape=[jax.ShapeDtypeStruct(slab.shape, f32), jax.ShapeDtypeStruct((images, rows, width), f32),
                   jax.ShapeDtypeStruct((images, rows, width), f32)],
        in_specs=[pl.BlockSpec(memory_space=pltpu.VMEM), anywhere, anywhere],
        out_specs=[pl.BlockSpec(memory_space=pltpu.VMEM), anywhere, anywhere],
        scratch_shapes=[
            pltpu.VMEM((2, width, columns), f32),
            pltpu.VMEM((2, width, columns), bf16), pltpu.VMEM((2, width, columns), bf16),
            full, full, act, act, act, act, act, act, act, act,
            pltpu.VMEM((own, 2, rows, 5 * LANES), f32), probs, probs,
            pltpu.VMEM((own, 2, rows, 2 * LANES), f32), full, full, full,
            pltpu.VMEM((width // LANES, inputs.shape[0], LANES), f32),
            pltpu.VMEM((8, width), f32), pltpu.VMEM((2, 1, 5 * LANES), f32), pltpu.VMEM((2, 1, hidden_local), f32),
            pltpu.VMEM((2, 8, hidden_local), f32),
            pltpu.VMEM((n, share, columns), f32), pltpu.VMEM((n - 1, share, columns), f32),
            dma((2, 3, n)), dma((2, n)), dma((2, n)), dma((2, n)),
            dma((2, n)), dma((2, n)), dma((2, n)), dma((2, n)),
            dma((width // LANES,)), dma((2, own)), dma((2, own)), dma((2, own)),
        ],
        compiler_params=pltpu.CompilerParams(
            collective_id=2, has_side_effects=True, vmem_limit_bytes=67043328),
        name="step",
    )(slab, inputs, cotangent)


def pack_attention(mixer, output):
    head = mixer.shape[2] // 3
    pair = 2 * head
    out = output.T
    q, k, v = mixer[:, 0], mixer[:, 1], mixer[:, 2]
    return jnp.concatenate([q[:, :pair], k[:, :pair], v[:, :pair], q[:, pair:], k[:, pair:], v[:, pair:],
                            out[:, pair:], out[:, :pair]], axis=1)


def unpack_attention(block, head):
    pair = 2 * head
    cut = [block[:, t * head:(t + 1) * head] for t in range(12)]
    mixer = jnp.stack([jnp.concatenate(t, axis=1) for t in (
        (cut[0], cut[1], cut[6]), (cut[2], cut[3], cut[7]), (cut[4], cut[5], cut[8]))], axis=1)
    output = jnp.concatenate([cut[10], cut[11], cut[9]], axis=1).T
    return mixer, output


SMALL = ("first_gain", "first_shift", "output_bias", "second_gain", "second_shift", "reduce_bias",
         "mixer_bias", "expand_bias")


def pack_small(values):
    return jnp.concatenate([values[name].reshape(-1) for name in SMALL])


def unpack_small(flat, like):
    out, start = {}, 0
    for name in SMALL:
        size = like[name].size
        out[name] = flat[start:start + size].reshape(like[name].shape)
        start += size
    return out


def adam_update(param, grad, momentum, variance, decay):
    momentum_next = beta_one * momentum + (1.0 - beta_one) * grad
    variance_next = beta_two * variance + (1.0 - beta_two) * grad * grad
    mean_hat = momentum_next / (1.0 - beta_one**step_count)
    square_hat = variance_next / (1.0 - beta_two**step_count)
    stepped = param - learn_rate * (mean_hat / (jnp.sqrt(square_hat) + adam_eps) + decay * param)
    return (stepped, momentum_next, variance_next)


NAMES = ("first_gain", "first_shift", "mixer_weight", "mixer_bias", "output_weight", "output_bias", "second_gain",
         "second_shift", "expand_weight", "expand_bias", "reduce_weight", "reduce_bias")
DECAYED = ("mixer_weight", "output_weight", "expand_weight", "reduce_weight")


def per_device(inputs, cotangent, *rest):
    if rest[0].shape[0] % 8 == 0:
        return one_kernel(inputs, cotangent, *rest)
    return three_kernels(inputs, cotangent, *rest)


def finish(params, momenta, variances, gradients, block_out, input_gradient):
    results = [adam_update(params[m], gradients[m], momenta[m], variances[m], weight_decay if m in DECAYED else 0.0)
               for m in NAMES]
    return (block_out, input_gradient, *(gradients[m] for m in NAMES), *(r[0] for r in results),
            *(r[1] for r in results), *(r[2] for r in results))


def one_kernel(inputs, cotangent, *rest):
    n = lax.axis_size("dp")
    images, length, width = inputs.shape
    scale = (n * images * length) ** (-0.5)
    params = dict(zip(NAMES, rest[:12]))
    momenta = dict(zip(NAMES, rest[12:24]))
    variances = dict(zip(NAMES, rest[24:]))
    share = params["first_gain"].shape[0]
    heads, piece = params["mixer_bias"].shape[1:]
    head = piece * n
    hidden_local = params["expand_weight"].shape[1]
    small = jnp.pad(pack_small(params).reshape(-1, share).T, ((0, 0), (0, LANES - 9)))
    slab = jnp.concatenate([
        pack_attention(params["mixer_weight"], params["output_weight"]), small,
        params["expand_weight"], params["reduce_weight"].T], axis=1)

    def tokens(v):
        return v.transpose(1, 0, 2).reshape(length * images, width)

    summed, block_out, input_gradient = run_step(slab, tokens(inputs), tokens(cotangent), n, heads, head, length)
    summed = summed * scale
    mixer, output = unpack_attention(summed[:, :6 * LANES], head)
    gradients = unpack_small(summed[:, 6 * LANES:6 * LANES + 9].T.reshape(-1), params)
    up = 7 * LANES
    gradients.update(mixer_weight=mixer, output_weight=output, expand_weight=summed[:, up:up + hidden_local],
                     reduce_weight=summed[:, up + hidden_local:].T)
    return finish(params, momenta, variances, gradients, block_out[:, :length], input_gradient[:, :length])


def three_kernels(inputs, cotangent, *rest):
    n = lax.axis_size("dp")
    scale = (n * inputs.shape[0] * inputs.shape[1]) ** (-0.5)
    params = dict(zip(NAMES, rest[:12]))
    momenta = dict(zip(NAMES, rest[12:24]))
    variances = dict(zip(NAMES, rest[24:]))
    share, width = params["first_gain"].shape[0], inputs.shape[2]
    heads, piece = params["mixer_bias"].shape[1:]
    head = piece * n
    hidden_local = params["expand_weight"].shape[1]
    end = 6 * LANES + 2 * hidden_local

    small = pack_small(params)
    count = small.shape[0]
    slab = jnp.concatenate([
        pack_attention(params["mixer_weight"], params["output_weight"]),
        params["expand_weight"], params["reduce_weight"].T,
        jnp.pad(small, (0, share * LANES - count)).reshape(share, LANES)], axis=1)
    columns = slab.shape[1]
    gathered = gather(slab, n)

    flat = gathered[:, :, :, end:].reshape(2, n, share * LANES)[:, :, :count]
    vectors = jnp.pad(flat[0, :, :6 * share].reshape(n, 6, share).transpose(1, 0, 2).reshape(6, width),
                      ((0, 2), (0, 0)))
    bias = flat[:, :, 6 * share:7 * share].reshape(2, n, 2, heads, piece).transpose(0, 2, 3, 1, 4)
    bias = bias.reshape(2, 2, heads * head)
    q, v, none = bias[:, 0], bias[:, 1], jnp.zeros((2, 2 * head), f32)
    mixed_bias = jnp.concatenate([q[:, :2 * head], none, v[:, :2 * head], q[:, 2 * head:], none[:, :head],
                                  v[:, 2 * head:], none[:, :head]], axis=1)[:, None]
    expand_bias = flat[:, :, 7 * share:].reshape(2, n, -1, piece).transpose(0, 2, 1, 3).reshape(2, 1, -1)

    base = (lax.axis_index("mp") * (inputs.shape[0] // 2)).astype(jnp.int32).reshape(1)
    block_out, input_gradient, grads, small_grads = run_layer(
        base, inputs, cotangent, gathered.reshape(2, width, columns), vectors, mixed_bias, expand_bias, heads, head)

    total = small_grads[:1, :6, :width].reshape(6, n, share).transpose(1, 0, 2).reshape(n, 6 * share)
    row = small_grads[:, 6, :5 * LANES]
    bias = jnp.stack([
        jnp.concatenate([row[:, :2 * head], row[:, 6 * head:7 * head]], axis=1),
        jnp.concatenate([row[:, 4 * head:6 * head], row[:, 8 * head:9 * head]], axis=1)], axis=1)
    bias = bias.reshape(2, 2, heads, n, piece).transpose(0, 3, 1, 2, 4).reshape(2, n, share)
    hidden = small_grads[:, 7].reshape(2, hidden_local // head, n, piece).transpose(0, 2, 1, 3).reshape(2, n, -1)
    packed = jnp.concatenate([jnp.broadcast_to(total[None], (2,) + total.shape), bias, hidden], axis=2)
    packed = jnp.pad(packed, ((0, 0), (0, 0), (0, share * LANES - count))).reshape(2, n, share, LANES)
    grads = lax.dynamic_update_slice(grads.reshape(2, n, share, columns), packed, (0, 0, 0, end))

    summed, block_out, input_gradient = scatter(grads, block_out, input_gradient, n)
    summed = summed * scale
    mixer, output = unpack_attention(summed[:, :6 * LANES], head)
    gradients = unpack_small(summed[:, end:].reshape(-1), params)
    gradients.update(mixer_weight=mixer, output_weight=output,
                     expand_weight=summed[:, 6 * LANES:6 * LANES + hidden_local],
                     reduce_weight=summed[:, 6 * LANES + hidden_local:end].T)
    return finish(params, momenta, variances, gradients, block_out, input_gradient)


def solution(mesh):
    images = P("dp", None, None)
    entries = (P("dp"), P("dp"), P("dp", None, "mp"), P(None, "mp", "dp"), P("mp", "dp"), P("dp"), P("dp"), P("dp"),
               P("dp", "mp"), P("mp", "dp"), P("mp", "dp"), P("dp"))
    return jax.shard_map(per_device, mesh=mesh, in_specs=(images, images) + entries * 3,
                         out_specs=(images, images) + entries * 4, check_vma=False)
```

```python
import functools
import heapq

import jax
import jax.numpy as jnp
from jax import lax
from jax.experimental import pallas as pl
from jax.experimental.pallas import tpu as pltpu
from jax.sharding import PartitionSpec as P

norm_eps = 1e-06
beta_one = 0.9
beta_two = 0.99
adam_eps = 1e-08
learn_rate = 0.05
weight_decay = 0.05
step_count = 3.0

LANES = 128
MASKED = -1e30
f32, bf16 = jnp.float32, jnp.bfloat16


def split(x):
    high = x.astype(bf16)
    return high, (x - high.astype(f32)).astype(bf16)


def dot(a, b, da, db):
    return lax.dot_general(a, b, (((da,), (db,)), ((), ())), preferred_element_type=f32)


def product(a, b, da, db):
    left = jnp.concatenate([a[0], a[0], a[1]], axis=da)
    right = jnp.concatenate([b[0], b[1], b[0]], axis=db)
    return dot(left, right, da, db)


def product_apart(a, b, da, db):
    n = b[0].shape[1 - db]
    both = dot(a[0], jnp.concatenate(b, axis=1 - db), da, db)
    return both[:, :n] + both[:, n:] + dot(a[1], b[0], da, db)


def layer_kernel(length, heads, head, base, x_ref, cot_ref, w_ref, vec_ref, mb_ref, eb_ref,
                 y_ref, gx_ref, g_ref, sg_ref,
                 whi, wlo, wsem, pad, mixed, probs_hi, probs_lo, joined,
                 fo_hi, fo_lo, so_hi, so_lo, cot_hi, cot_lo, gm_hi, gm_lo, part, part2):
    step = pl.program_id(0)
    rows, width = pad.shape[1], pad.shape[2]
    local = heads * head
    qkv = 5 * LANES
    hidden_local = eb_ref.shape[-1]
    attn = 6 * LANES
    up, down, end = attn, attn + hidden_local, attn + 2 * hidden_local

    @pl.when(step == 0)
    def _():
        for c in range(2):
            pltpu.make_async_copy(w_ref.at[c], g_ref.at[c], wsem.at[c]).start()
        pad[...] = jnp.zeros_like(pad)
        sg_ref[...] = jnp.zeros_like(sg_ref)
        for c in range(2):
            pltpu.make_async_copy(w_ref.at[c], g_ref.at[c], wsem.at[c]).wait()

        def convert(t, _):
            c, r = t // (width // 16), t % (width // 16)
            at = pl.ds(pl.multiple_of(r * 16, 16), 16)
            high, low = split(g_ref[c, at, 0:end])
            whi[c, at, :] = high
            wlo[c, at, :] = low
            g_ref[c, at, :] = jnp.zeros((16, g_ref.shape[2]), f32)
            return 0

        lax.fori_loop(0, 2 * (width // 16), convert, 0)

    def weight(c, lo, hi):
        return whi[c, :, lo:hi], wlo[c, :, lo:hi]

    def vec(r):
        return vec_ref[r:r + 1, :]

    def normalize(v):
        center = v - jnp.mean(v, axis=-1, keepdims=True)
        inverse = lax.rsqrt(jnp.mean(center * center, axis=-1, keepdims=True) + norm_eps)
        return center * inverse, inverse

    def norm_back(grad, normed, inverse, gain):
        scaled = grad * gain
        return inverse * (scaled - jnp.mean(scaled, axis=-1, keepdims=True)
                          - normed * jnp.mean(scaled * normed, axis=-1, keepdims=True))

    def total(v):
        return jnp.sum(v, axis=0, keepdims=True)

    pad[0, 0:length, :] = x_ref[0]
    pad[1, 0:length, :] = cot_ref[0]
    x, cot = pad[0], pad[1]
    cot_hi[...], cot_lo[...] = split(cot)
    first, first_inverse = normalize(x)
    fo_hi[...], fo_lo[...] = split(first * vec(0) + vec(1))

    lane = lax.broadcasted_iota(jnp.int32, (rows, LANES), 1)
    sides = (lane < head, lane >= head)
    column = lax.broadcasted_iota(jnp.int32, (rows, rows), 1)
    score_scale = head ** (-0.5)

    def side(v, s):
        return jnp.where(sides[s], v, 0.0)

    def swap(v):
        return pltpu.roll(v, head, 1)

    def windows(c):
        w = [mixed[c, :, t * LANES:(t + 1) * LANES] for t in range(5)]
        third = side(w[3], 0) * score_scale, side(swap(w[3]), 0), side(w[4], 0)
        return [
            (side(w[0], 0) * score_scale, side(w[1], 0), side(w[2], 0)),
            (side(w[0], 1) * score_scale, side(w[1], 1), side(w[2], 1)),
            third,
        ]

    part[...] = jnp.zeros_like(part)

    def attend(c, _):
        mixed[c] = product((fo_hi[...], fo_lo[...]), weight(c, 0, qkv), 1, 0) + mb_ref[c]
        outs = []
        for h, (q, k, v) in enumerate(windows(c)):
            scores = product(split(q), split(k), 1, 1)
            scores = jnp.where(column < length, scores, MASKED)
            expon = jnp.exp(scores - jnp.max(scores, axis=-1, keepdims=True))
            probs = split(expon / jnp.sum(expon, axis=-1, keepdims=True))
            probs_hi[c, h], probs_lo[c, h] = probs
            outs.append(product_apart(probs, split(v), 1, 0))
        joined[c] = jnp.concatenate([swap(outs[2]), outs[0] + outs[1]], axis=1)
        part[...] += product(split(joined[c]), weight(c, 4 * LANES, attn), 1, 1)
        return 0

    lax.fori_loop(0, 2, attend, 0)
    middle = x + part[...] + vec(2)
    second, second_inverse = normalize(middle)
    so_hi[...], so_lo[...] = split(second * vec(3) + vec(4))

    part[...] = middle + vec(5)
    part2[...] = jnp.zeros_like(part2)

    def feed(c, _):
        so = (so_hi[...], so_lo[...])
        co = (cot_hi[...], cot_lo[...])
        hidden = product(so, weight(c, up, down), 1, 0) + eb_ref[c]
        share = 0.5 * (1.0 + lax.erf(hidden * (0.5 ** 0.5)))
        active = split(hidden * share)
        slope = share + hidden * jnp.exp(-0.5 * hidden * hidden) * 0.3989422804014327
        part[...] += product(active, weight(c, down, end), 1, 1)
        g_ref[c, :, down:end] += product(co, active, 0, 0)
        grad = product(co, weight(c, down, end), 1, 0) * slope
        sg_ref[c, 7:8, 0:hidden_local] += total(grad)
        grad = split(grad)
        g_ref[c, :, up:down] += product(so, grad, 0, 0)
        part2[...] += product(grad, weight(c, up, down), 1, 1)
        return 0

    lax.fori_loop(0, 2, feed, 0)
    y_ref[0] = part[0:length, :]

    grad_second = part2[...]
    sg_ref[0, 3:4, 0:width] += total(grad_second * second)
    sg_ref[0, 4:5, 0:width] += total(grad_second)
    sg_ref[0, 5:6, 0:width] += total(cot)
    grad_middle = cot + norm_back(grad_second, second, second_inverse, vec(3))
    sg_ref[0, 2:3, 0:width] += total(grad_middle)
    gm_hi[...], gm_lo[...] = split(grad_middle)
    part2[...] = grad_middle

    part[...] = jnp.zeros_like(part)

    def attend_back(c, _):
        gm = (gm_hi[...], gm_lo[...])
        fo = (fo_hi[...], fo_lo[...])
        grad_heads = product(gm, weight(c, 4 * LANES, attn), 1, 0)
        g_ref[c, :, 4 * LANES:attn] += product(gm, split(joined[c]), 0, 0)
        pair, single = grad_heads[:, LANES:], swap(grad_heads[:, :LANES])
        pair_out, single_out = joined[c, :, LANES:], swap(joined[c, :, :LANES])
        grad_outs = (side(pair, 0), side(pair, 1), side(single, 0))
        outs = (pair_out, pair_out, single_out)
        grads = []
        for h, (q, k, v) in enumerate(windows(c)):
            grad_out = grad_outs[h]
            row = jnp.sum(grad_out * outs[h], axis=-1, keepdims=True)
            grad_out = split(grad_out)
            grad_probs = product(grad_out, split(v), 1, 1)
            probs = (probs_hi[c, h], probs_lo[c, h])
            grad_v = product_apart(probs, grad_out, 0, 0)
            grad_scores = split((probs[0].astype(f32) + probs[1].astype(f32)) * (grad_probs - row))
            grad_q = product_apart(grad_scores, split(k), 1, 0) * score_scale
            grad_k = product_apart(grad_scores, split(q), 0, 0)
            grads.append((grad_q, grad_k, grad_v))
        one, two, three = grads
        grad_mixed = jnp.concatenate(
            [one[0] + two[0], one[1] + two[1], one[2] + two[2], three[0] + swap(three[1]), three[2]], axis=1)
        sg_ref[c, 6:7, 0:qkv] += total(grad_mixed)
        grad_mixed = split(grad_mixed)
        g_ref[c, :, 0:qkv] += product(fo, grad_mixed, 0, 0)
        part[...] += product(grad_mixed, weight(c, 0, qkv), 1, 1)
        return 0

    lax.fori_loop(0, 2, attend_back, 0)
    grad_first = part[...]
    sg_ref[0, 0:1, 0:width] += total(grad_first * first)
    sg_ref[0, 1:2, 0:width] += total(grad_first)
    gx_ref[0] = (part2[...] + norm_back(grad_first, first, first_inverse, vec(0)))[0:length, :]


def run_layer(base, inputs, cotangent, weights, vectors, mixed_bias, expand_bias, heads, head):
    images, length, width = inputs.shape
    own = images // 2
    rows = -(-length // 16) * 16
    columns = weights.shape[-1]
    hidden_local = expand_bias.shape[-1]
    end = 6 * LANES + 2 * hidden_local
    image = pl.BlockSpec((1, length, width), lambda i, b: (b[0] + i, 0, 0))

    def whole(shape):
        return pl.BlockSpec(shape, lambda i, b: (0,) * len(shape))

    act = pltpu.VMEM((rows, width), bf16)
    return pl.pallas_call(
        functools.partial(layer_kernel, length, heads, head),
        grid_spec=pltpu.PrefetchScalarGridSpec(
            num_scalar_prefetch=1,
            grid=(own,),
            in_specs=[image, image, pl.BlockSpec(memory_space=pl.ANY), whole(vectors.shape),
                      whole(mixed_bias.shape), whole(expand_bias.shape)],
            out_specs=[image, image, whole((2, width, columns)), whole((2, 8, hidden_local))],
            scratch_shapes=[
                pltpu.VMEM((2, width, end), bf16), pltpu.VMEM((2, width, end), bf16),
                pltpu.SemaphoreType.DMA((2,)),
                pltpu.VMEM((2, rows, width), f32),
                pltpu.VMEM((2, rows, 5 * LANES), f32),
                pltpu.VMEM((2, heads, rows, rows), bf16), pltpu.VMEM((2, heads, rows, rows), bf16),
                pltpu.VMEM((2, rows, 2 * LANES), f32),
                act, act, act, act, act, act, act, act,
                pltpu.VMEM((rows, width), f32), pltpu.VMEM((rows, width), f32),
            ],
        ),
        out_shape=[
            jax.ShapeDtypeStruct(inputs.shape, f32), jax.ShapeDtypeStruct(inputs.shape, f32),
            jax.ShapeDtypeStruct((2, width, columns), f32), jax.ShapeDtypeStruct((2, 8, hidden_local), f32),
        ],
        compiler_params=pltpu.CompilerParams(
            dimension_semantics=("arbitrary",), vmem_limit_bytes=60 * 2**20),
        name="layer",
    )(base, inputs, cotangent, weights, vectors, mixed_bias, expand_bias)


def rings(n):
    side = max(k for k in range(1, n + 1) if n % (k * k) == 0 and n // (k * k) >= k)
    return n // (side * side), side, side


def place(sizes):
    first, side, _ = sizes
    core, me = lax.axis_index("mp"), lax.axis_index("dp")
    a, b, c = lax.div(me, side * side), lax.rem(lax.div(me, side), side), lax.rem(me, side)
    firsts = [lax.rem(a + i, first) * (side * side) for i in range(first)]
    bs = [lax.rem(b + j, side) for j in range(side)]
    cs = [lax.rem(c + j, side) for j in range(side)]
    cores = {"mine": core, "other": 1 - core}
    pairs = {}
    for of, which in cores.items():
        for j in range(side):
            for k in range(side):
                ahead_b = bs[j] * which + bs[k] * (1 - which)
                ahead_c = cs[k] * which + cs[j] * (1 - which)
                pairs[of, j, k] = ahead_b * side + ahead_c
    places = {(of, i, j, k): firsts[i] + pairs[of, j, k]
              for of in cores for i in range(first) for j in range(side) for k in range(side)}

    def at(slab, sign=1, of="mine"):
        i, j, k = slab
        return places[of, (sign * i) % first, (sign * j) % side, (sign * k) % side]

    return core, at


UNITS = ((1, 0, 0), (0, 1, 0), (0, 0, 1))


def plus(slab, unit):
    return tuple(s + u for s, u in zip(slab, unit))


def sends(slab, sizes):
    out = [(0, (i, 0, 0), (i, 0, 0)) for i in range(1, sizes[0])] if not any(slab) else []
    for r in (1, 2):
        if not any(slab[r + 1:]) and slab[r] + 1 < sizes[r]:
            out.append((r, UNITS[r], plus(slab, UNITS[r])))
    return out


def sources(slab, sizes):
    out = [(i, 0, 0) for i in range(1, sizes[0])] if not any(slab) else []
    for r in (1, 2):
        if not any(slab[r + 1:]) and slab[r] + 1 < sizes[r]:
            out.append(plus(slab, UNITS[r]))
    return out


def hop(slab):
    r = max(q for q in range(3) if slab[q])
    return slab if r == 0 else UNITS[r]


def arrival_order(sizes):
    cost, free, heap, order = (2.0, 1.5, 1.5), [0.0] * 3, [(0.0, (0, 0, 0))], []
    while heap:
        now, slab = heapq.heappop(heap)
        order.append(slab)
        for r, _, there in sends(slab, sizes):
            free[r] = max(now, free[r]) + cost[r]
            heapq.heappush(heap, (free[r] + 1.0, there))
    return order


def slab_id(slab, sizes):
    return (slab[0] * sizes[1] + slab[1]) * sizes[2] + slab[2]


def greet(core, at, sizes):
    barrier = pltpu.get_barrier_semaphore()
    backs = [(i, 0, 0) for i in range(1, sizes[0])] + [UNITS[1], UNITS[2]]
    for steps in backs:
        pl.semaphore_signal(barrier, inc=1, device_id={"dp": at(steps, -1)})
    pl.semaphore_signal(barrier, inc=1, device_id={"mp": 1 - core})
    pl.semaphore_wait(barrier, len(backs) + 1)


def gather_kernel(sizes, slab_ref, out_ref, send_sem, recv_sem, swap_send, swap_recv, own_sem):
    core, at = place(sizes)
    number = functools.partial(slab_id, sizes=sizes)
    greet(core, at, sizes)

    def landing(slab, of):
        return out_ref.at[core if of == "mine" else 1 - core, at(slab, -1, of)]

    started = []
    own = pltpu.make_async_copy(slab_ref, landing((0, 0, 0), "mine"), own_sem)
    for slab in arrival_order(sizes):
        spot = landing(slab, "mine")
        if any(slab):
            pltpu.make_async_remote_copy(
                src_ref=spot, dst_ref=spot, send_sem=send_sem.at[0, 0], recv_sem=recv_sem.at[number(slab)],
                device_id={"mp": 1 - core}).wait_recv()
        source = spot if any(slab) else slab_ref
        for r, steps, there in reversed(sends(slab, sizes)):
            copy = pltpu.make_async_remote_copy(
                src_ref=source, dst_ref=spot, send_sem=send_sem.at[r, number(there)],
                recv_sem=recv_sem.at[number(there)], device_id={"dp": at(steps)})
            copy.start()
            started.append(copy)
        copy = pltpu.make_async_remote_copy(
            src_ref=source, dst_ref=spot, send_sem=swap_send.at[number(slab)], recv_sem=swap_recv.at[number(slab)],
            device_id={"mp": 1 - core})
        copy.start()
        started.append(copy)
        if not any(slab):
            own.start()
    for slab in arrival_order(sizes):
        spot = landing(slab, "other")
        pltpu.make_async_remote_copy(
            src_ref=spot, dst_ref=spot, send_sem=swap_send.at[0], recv_sem=swap_recv.at[number(slab)],
            device_id={"mp": 1 - core}).wait_recv()
    for copy in started:
        copy.wait_send()
    own.wait()


def gather(slab, n):
    sizes = rings(n)
    return pl.pallas_call(
        functools.partial(gather_kernel, sizes),
        out_shape=jax.ShapeDtypeStruct((2, n) + slab.shape, f32),
        in_specs=[pl.BlockSpec(memory_space=pltpu.VMEM)],
        out_specs=pl.BlockSpec(memory_space=pl.ANY),
        scratch_shapes=[
            pltpu.SemaphoreType.DMA((3, n)), pltpu.SemaphoreType.DMA((n,)),
            pltpu.SemaphoreType.DMA((n,)), pltpu.SemaphoreType.DMA((n,)), pltpu.SemaphoreType.DMA,
        ],
        compiler_params=pltpu.CompilerParams(collective_id=0, has_side_effects=True),
        name="gather",
    )(slab)


def scatter_kernel(sizes, g_ref, y_in, gx_in, out_ref, y_ref, gx_ref,
                   acc, swapped, landed, load_sem, send_sem, recv_sem, swap_send, swap_recv, image_send, image_recv):
    del y_in, gx_in
    core, at = place(sizes)
    number = functools.partial(slab_id, sizes=sizes)
    greet(core, at, sizes)
    first, side, _ = sizes
    order = [(i, j, k) for k in reversed(range(side)) for j in reversed(range(side)) for i in reversed(range(first))]
    own = y_ref.shape[0] // 2
    started, loads, images = [], {}, []
    for slab in order:
        s = number(slab)
        copy = pltpu.make_async_remote_copy(
            src_ref=g_ref.at[1 - core, at(slab, 1, "other")], dst_ref=swapped.at[s],
            send_sem=swap_send.at[s], recv_sem=swap_recv.at[s], device_id={"mp": 1 - core})
        copy.start()
        started.append(copy)
        loads[slab] = pltpu.make_async_copy(g_ref.at[core, at(slab)], acc.at[s], load_sem.at[s])
        loads[slab].start()
    for t, ref in enumerate((y_ref, gx_ref)):
        mine = ref.at[pl.ds(core * own, own)]
        copy = pltpu.make_async_remote_copy(
            src_ref=mine, dst_ref=mine, send_sem=image_send.at[t], recv_sem=image_recv.at[t],
            device_id={"mp": 1 - core})
        copy.start()
        started.append(copy)
        theirs = ref.at[pl.ds((1 - core) * own, own)]
        images.append(pltpu.make_async_remote_copy(
            src_ref=theirs, dst_ref=theirs, send_sem=image_send.at[t], recv_sem=image_recv.at[t],
            device_id={"mp": 1 - core}))

    def arrived(buffer, spot, sem):
        pltpu.make_async_remote_copy(
            src_ref=buffer.at[spot], dst_ref=buffer.at[spot], send_sem=swap_send.at[0], recv_sem=sem,
            device_id={"mp": 1 - core}).wait_recv()
        return buffer[spot]

    for slab in order:
        s = number(slab)
        loads[slab].wait()
        value = acc[s] + arrived(swapped, s, swap_recv.at[s])
        for other in sources(slab, sizes):
            spot = number(other)
            value = value + arrived(landed, spot - 1, recv_sem.at[spot])
        if any(slab):
            acc[s] = value
            copy = pltpu.make_async_remote_copy(
                src_ref=acc.at[s], dst_ref=landed.at[s - 1], send_sem=send_sem.at[s], recv_sem=recv_sem.at[s],
                device_id={"dp": at(hop(slab))})
            copy.start()
            started.append(copy)
        else:
            out_ref[...] = value
    for copy in images:
        copy.wait_recv()
    for copy in started:
        copy.wait_send()


def scatter(grads, block_out, input_gradient, n):
    sizes = rings(n)
    slab = grads.shape[2:]
    anywhere = pl.BlockSpec(memory_space=pl.ANY)
    return pl.pallas_call(
        functools.partial(scatter_kernel, sizes),
        out_shape=[jax.ShapeDtypeStruct(slab, f32), jax.ShapeDtypeStruct(block_out.shape, f32),
                   jax.ShapeDtypeStruct(input_gradient.shape, f32)],
        in_specs=[anywhere] * 3,
        out_specs=[pl.BlockSpec(memory_space=pltpu.VMEM), anywhere, anywhere],
        input_output_aliases={1: 1, 2: 2},
        scratch_shapes=[
            pltpu.VMEM((n,) + slab, f32), pltpu.VMEM((n,) + slab, f32), pltpu.VMEM((n - 1,) + slab, f32),
            pltpu.SemaphoreType.DMA((n,)), pltpu.SemaphoreType.DMA((n,)), pltpu.SemaphoreType.DMA((n,)),
            pltpu.SemaphoreType.DMA((n,)), pltpu.SemaphoreType.DMA((n,)),
            pltpu.SemaphoreType.DMA((2,)), pltpu.SemaphoreType.DMA((2,)),
        ],
        compiler_params=pltpu.CompilerParams(
            collective_id=1, has_side_effects=True, vmem_limit_bytes=60 * 2**20),
        name="scatter",
    )(grads, block_out, input_gradient)


def spread(count, slots, lead):
    return [min(slots - 1, lead + (e * (slots - lead)) // count) for e in range(count)]


def step_kernel(sizes, length, heads, head, mixer_ref, turned_ref, small_ref, up_ref, down_ref, x_ref, cot_ref, out_ref, y_ref, gx_ref,
                slab_ref, buf, whi, wlo, xs, cots, fo_hi, fo_lo, so_hi, so_lo, cot_hi, cot_lo, gm_hi, gm_lo,
                mixed, probs_hi, probs_lo, joined, mid, back, yb, staged, vec_ref, bias_ref, hidden_bias, small_grads,
                swapped, landed, send_sem, recv_sem, swap_send, swap_recv,
                push_send, push_recv, trade_send, trade_recv, stage_sem, image_sem, image_send, image_recv):
    core, at = place(sizes)
    number = functools.partial(slab_id, sizes=sizes)
    n = sizes[0] * sizes[1] * sizes[2]
    own, rows, width = xs.shape
    share = up_ref.shape[0]
    hidden_local = hidden_bias.shape[-1]
    qkv, attn = 5 * LANES, 6 * LANES
    small, up = attn, attn + LANES
    down, end = up + hidden_local, up + 2 * hidden_local
    spans = ((0, up), (up, end))
    partner = {"mp": 1 - core}

    def block(slab, sign, of):
        return pl.ds(pl.multiple_of(at(slab, sign, of) * share, 8), share)

    def span(p):
        return slice(*spans[p])

    def landing(p, slab, of):
        return buf.at[core if of == "mine" else 1 - core, block(slab, -1, of), span(p)]

    def gather_event(p, slab, along=(0, 1, 2), swap=True):
        spot = landing(p, slab, "mine")
        if any(slab):
            pltpu.make_async_remote_copy(
                src_ref=spot, dst_ref=spot, send_sem=send_sem.at[p, 0, 0], recv_sem=recv_sem.at[p, number(slab)],
                device_id=partner).wait_recv()
        source = spot if any(slab) else slab_ref.at[:, span(p)]
        for r, steps, there in reversed(sends(slab, sizes)):
            if r in along:
                pltpu.make_async_remote_copy(
                    src_ref=source, dst_ref=spot, send_sem=send_sem.at[p, r, number(there)],
                    recv_sem=recv_sem.at[p, number(there)], device_id={"dp": at(steps)}).start()
        if swap:
            pltpu.make_async_remote_copy(
                src_ref=source, dst_ref=spot, send_sem=swap_send.at[p, number(slab)],
                recv_sem=swap_recv.at[p, number(slab)], device_id=partner).start()

    def gather_end(p):
        for slab in order:
            spot = landing(p, slab, "other")
            pltpu.make_async_remote_copy(
                src_ref=spot, dst_ref=spot, send_sem=swap_send.at[p, 0], recv_sem=swap_recv.at[p, number(slab)],
                device_id=partner).wait_recv()
        for slab in order:
            spot = landing(p, slab, "mine")
            for r, _, there in sends(slab, sizes):
                pltpu.make_async_remote_copy(
                    src_ref=spot, dst_ref=spot, send_sem=send_sem.at[p, r, number(there)],
                    recv_sem=recv_sem.at[p, 0], device_id=partner).wait_send()
            pltpu.make_async_remote_copy(
                src_ref=spot, dst_ref=spot, send_sem=swap_send.at[p, number(slab)], recv_sem=swap_recv.at[p, 0],
                device_id=partner).wait_send()

    order = arrival_order(sizes)

    first_size, side_size, _ = sizes
    back_order = [(i, j, k) for k in reversed(range(side_size)) for j in reversed(range(side_size))
                  for i in reversed(range(first_size))]

    def trade(p, slab):
        s = number(slab)
        return pltpu.make_async_remote_copy(
            src_ref=buf.at[1 - core, block(slab, 1, "other"), span(p)], dst_ref=swapped.at[s, :, span(p)],
            send_sem=trade_send.at[p, s], recv_sem=trade_recv.at[p, s], device_id=partner)

    def scatter_start(p):
        for slab in back_order:
            trade(p, slab).start()

    def arrived(buffer, spot, p, sem):
        ref = buffer.at[spot, :, span(p)]
        pltpu.make_async_remote_copy(
            src_ref=ref, dst_ref=ref, send_sem=trade_send.at[p, 0], recv_sem=sem, device_id=partner).wait_recv()
        return ref[...]

    def push(p, slab):
        s = number(slab)
        return pltpu.make_async_remote_copy(
            src_ref=buf.at[core, block(slab, 1, "mine"), span(p)], dst_ref=landed.at[s - 1, :, span(p)],
            send_sem=push_send.at[p, s], recv_sem=push_recv.at[p, s], device_id={"dp": at(hop(slab))})

    def scatter_event(p, slab):
        s = number(slab)
        here = (core, block(slab, 1, "mine"), span(p))
        value = buf[here] + arrived(swapped, s, p, trade_recv.at[p, s])
        for other in sources(slab, sizes):
            spot = number(other)
            value = value + arrived(landed, spot - 1, p, push_recv.at[p, spot])
        if any(slab):
            buf[here] = value
            push(p, slab).start()
        else:
            out_ref[:, span(p)] = value

    def scatter_end(p):
        for slab in back_order:
            trade(p, slab).wait_send()
            if any(slab):
                push(p, slab).wait_send()

    def image_copies(t, source, ref, i):
        spot = ref.at[core * own + i]
        keep = pltpu.make_async_copy(source.at[i], spot, image_sem.at[t, i])
        give = pltpu.make_async_remote_copy(
            src_ref=source.at[i], dst_ref=spot, send_sem=image_send.at[t, i], recv_sem=image_recv.at[t, i],
            device_id=partner)
        theirs = ref.at[(1 - core) * own + i]
        take = pltpu.make_async_remote_copy(
            src_ref=theirs, dst_ref=theirs, send_sem=image_send.at[t, i], recv_sem=image_recv.at[t, i],
            device_id=partner)
        return keep, give, take

    def weight(c, lo, hi):
        return whi[c, :, lo:hi], wlo[c, :, lo:hi]

    def vec(r):
        return vec_ref[r:r + 1, :]

    def normalize(v):
        center = v - jnp.mean(v, axis=-1, keepdims=True)
        inverse = lax.rsqrt(jnp.mean(center * center, axis=-1, keepdims=True) + norm_eps)
        return center * inverse, inverse

    def norm_back(grad, normed, inverse, gain):
        scaled = grad * gain
        return inverse * (scaled - jnp.mean(scaled, axis=-1, keepdims=True)
                          - normed * jnp.mean(scaled * normed, axis=-1, keepdims=True))

    def total(v):
        return jnp.sum(v, axis=0, keepdims=True)

    def convert(lo, hi):
        def body(t, _):
            c, r = t // (width // 16), t % (width // 16)
            here = pl.ds(pl.multiple_of(r * 16, 16), 16)
            high, low = split(buf[c, here, lo:hi])
            whi[c, here, lo:hi] = high
            wlo[c, here, lo:hi] = low
            buf[c, here, lo:hi] = jnp.zeros((16, hi - lo), f32)
            return 0

        lax.fori_loop(0, 2 * (width // 16), body, 0)

    def thirds(v):
        high = v.astype(bf16)
        v = v - high.astype(f32)
        middle_term = v.astype(bf16)
        return high, middle_term, (v - middle_term.astype(f32)).astype(bf16)

    def moved(v, onehot, dim):
        return sum(dot(term, onehot, 1, dim) for term in reversed(thirds(v)))

    piece = head // n
    entry = lax.broadcasted_iota(jnp.int32, (width, LANES), 0)
    owner, inner = entry // share, entry % share
    target = lax.broadcasted_iota(jnp.int32, (width, LANES), 1)

    def attention_bias_at(t):
        kind, which = inner // (heads * piece), (inner // piece) % heads
        window = jnp.where(kind == 0, jnp.where(which < 2, 0, 3), jnp.where(which < 2, 2, 4))
        place_in = (which % 2) * head + owner * piece + inner % piece
        return ((window == t) & (place_in == target)).astype(f32).astype(bf16)

    def hidden_bias_at(half, t):
        flat = inner + half * share
        place_in = (flat // piece) * head + owner * piece + flat % piece
        return (place_in == target + t * LANES).astype(f32).astype(bf16)

    pair = 2 * head
    q, k, v = (mixer_ref[t] for t in range(3))
    turned = turned_ref[...]
    slab_ref[...] = jnp.concatenate(
        [q[:, :pair], k[:, :pair], v[:, :pair], q[:, pair:], k[:, pair:], v[:, pair:], turned[:, pair:], turned[:, :pair],
         small_ref[...], up_ref[...], down_ref[...]], axis=1)
    greet(core, at, sizes)
    gather_event(0, (0, 0, 0))
    gather_event(1, (0, 0, 0), (0,), False)
    staging = []
    tiles = width // LANES
    for t in range(tiles):
        staging.append(pltpu.make_async_copy(x_ref.at[:, t * LANES:(t + 1) * LANES], staged.at[t], stage_sem.at[t]))
        staging[-1].start()
    buf[core, block((0, 0, 0), 1, "mine"), :] = slab_ref[...]
    xs[...] = jnp.zeros_like(xs)
    cots[...] = jnp.zeros_like(cots)
    small_grads[...] = jnp.zeros_like(small_grads)
    for source, sink in ((x_ref, xs), (cot_ref, cots)):
        for t in range(tiles):
            lanes = slice(t * LANES, (t + 1) * LANES)
            copy = pltpu.make_async_copy(source.at[:, lanes], staged.at[t], stage_sem.at[t])
            if sink is cots:
                copy.start()
            copy.wait()
            for i in range(own):
                sink[i, 0:length, lanes] = staged[t, pl.ds(core * own + i, length, stride=2 * own), :]

    for slab in order[1:]:
        gather_event(0, slab)
    gather_event(1, (0, 0, 0), (1, 2))
    for i in range(own):
        cot_hi[i], cot_lo[i] = split(cots[i])
    gather_end(0)
    for c in range(2):
        turned = buf[c, :, small:up].T
        if c == 0:
            vec_ref[...] = turned[0:8, :]
        packed = turned[0:16, :]
        for t in range(5):
            bias_ref[c, :, t * LANES:(t + 1) * LANES] = moved(packed[6:7], attention_bias_at(t), 0)
        for t in range(hidden_local // LANES):
            hidden_bias[c, :, t * LANES:(t + 1) * LANES] = (
                moved(packed[7:8], hidden_bias_at(0, t), 0) + moved(packed[8:9], hidden_bias_at(1, t), 0))
    convert(0, attn)

    lane = lax.broadcasted_iota(jnp.int32, (rows, LANES), 1)
    sides = (lane < head, lane >= head)
    column = lax.broadcasted_iota(jnp.int32, (rows, rows), 1)
    score_scale = head ** (-0.5)

    def side(v, s):
        return jnp.where(sides[s], v, 0.0)

    def swap(v):
        return pltpu.roll(v, head, 1)

    def windows(i, c):
        w = [mixed[i, c, :, t * LANES:(t + 1) * LANES] for t in range(5)]
        return [
            (side(w[0], 0) * score_scale, side(w[1], 0), side(w[2], 0)),
            (side(w[0], 1) * score_scale, side(w[1], 1), side(w[2], 1)),
            (side(w[3], 0) * score_scale, side(swap(w[3]), 0), side(w[4], 0)),
        ]

    def serve(t, plan, event):
        for slot in sorted({slot for slot, _ in plan}):
            @pl.when(t == slot)
            def _(slot=slot):
                for when, slab in plan:
                    if when == slot:
                        event(1, slab)

    gather_plan = list(zip(spread(len(order) - 1, 2 * own, 0), order[1:]))

    def attend(t, _):
        i, c = t // 2, t % 2

        @pl.when(c == 0)
        def _():
            normed, _ = normalize(xs[i])
            fo_hi[i], fo_lo[i] = split(normed * vec(0) + vec(1))
            mid[i] = xs[i] + vec(2)

        serve(t, gather_plan, gather_event)
        mixed[i, c] = product((fo_hi[i], fo_lo[i]), weight(c, 0, qkv), 1, 0) + bias_ref[c]
        outs = []
        for h, (q, k, v) in enumerate(windows(i, c)):
            scores = product(split(q), split(k), 1, 1)
            scores = jnp.where(column < length, scores, MASKED)
            expon = jnp.exp(scores - jnp.max(scores, axis=-1, keepdims=True))
            probs = split(expon / jnp.sum(expon, axis=-1, keepdims=True))
            probs_hi[i, c, h], probs_lo[i, c, h] = probs
            outs.append(product_apart(probs, split(v), 1, 0))
        joined[i, c] = jnp.concatenate([swap(outs[2]), outs[0] + outs[1]], axis=1)
        mid[i] += product(split(joined[i, c]), weight(c, 4 * LANES, attn), 1, 1)
        return 0

    lax.fori_loop(0, 2 * own, attend, 0)
    gather_end(1)
    convert(up, end)

    def feed(t, _):
        i, c = t // 2, t % 2

        @pl.when(c == 0)
        def _():
            second, _ = normalize(mid[i])
            so_hi[i], so_lo[i] = split(second * vec(3) + vec(4))
            yb[i] = mid[i] + vec(5)
            back[i] = jnp.zeros((rows, width), f32)

        so = (so_hi[i], so_lo[i])
        co = (cot_hi[i], cot_lo[i])
        hidden = product(so, weight(c, up, down), 1, 0) + hidden_bias[c]
        portion = 0.5 * (1.0 + lax.erf(hidden * (0.5 ** 0.5)))
        active = split(hidden * portion)
        slope = portion + hidden * jnp.exp(-0.5 * hidden * hidden) * 0.3989422804014327
        yb[i] += product(active, weight(c, down, end), 1, 1)
        buf[c, :, down:end] += product(co, active, 0, 0)
        grad = product(co, weight(c, down, end), 1, 0) * slope
        small_grads[c, 7:8, 0:hidden_local] += total(grad)
        grad = split(grad)
        buf[c, :, up:down] += product(so, grad, 0, 0)
        back[i] += product(grad, weight(c, up, down), 1, 1)

        @pl.when(c == 1)
        def _():
            cot = cots[i]
            second, second_inverse = normalize(mid[i])
            grad_second = back[i]
            small_grads[0, 3:4, 0:width] += total(grad_second * second)
            small_grads[0, 4:5, 0:width] += total(grad_second)
            small_grads[0, 5:6, 0:width] += total(cot)
            grad_middle = cot + norm_back(grad_second, second, second_inverse, vec(3))
            small_grads[0, 2:3, 0:width] += total(grad_middle)
            gm_hi[i], gm_lo[i] = split(grad_middle)
            back[i] = grad_middle
            mid[i] = jnp.zeros((rows, width), f32)
            keep, give, _ = image_copies(0, yb, y_ref, i)
            keep.start()
            give.start()

        return 0

    lax.fori_loop(0, 2 * own, feed, 0)

    scatter_start(1)
    scatter_plan = list(zip(spread(len(back_order) - 1, 2 * own, 1), back_order[:-1]))

    def attend_back(t, _):
        i, c = t // 2, t % 2
        serve(t, scatter_plan, scatter_event)
        gm = (gm_hi[i], gm_lo[i])
        fo = (fo_hi[i], fo_lo[i])
        grad_heads = product(gm, weight(c, 4 * LANES, attn), 1, 0)
        buf[c, :, 4 * LANES:attn] += product(gm, split(joined[i, c]), 0, 0)
        pair, single = grad_heads[:, LANES:], swap(grad_heads[:, :LANES])
        pair_out, single_out = joined[i, c, :, LANES:], swap(joined[i, c, :, :LANES])
        grad_outs = (side(pair, 0), side(pair, 1), side(single, 0))
        outs = (pair_out, pair_out, single_out)
        grads = []
        for h, (q, k, v) in enumerate(windows(i, c)):
            grad_out = grad_outs[h]
            row = jnp.sum(grad_out * outs[h], axis=-1, keepdims=True)
            grad_out = split(grad_out)
            grad_probs = product(grad_out, split(v), 1, 1)
            probs = (probs_hi[i, c, h], probs_lo[i, c, h])
            grad_v = product_apart(probs, grad_out, 0, 0)
            grad_scores = split((probs[0].astype(f32) + probs[1].astype(f32)) * (grad_probs - row))
            grad_q = product_apart(grad_scores, split(k), 1, 0) * score_scale
            grad_k = product_apart(grad_scores, split(q), 0, 0)
            grads.append((grad_q, grad_k, grad_v))
        one, two, three = grads
        grad_mixed = jnp.concatenate(
            [one[0] + two[0], one[1] + two[1], one[2] + two[2], three[0] + swap(three[1]), three[2]], axis=1)
        small_grads[c, 6:7, 0:qkv] += total(grad_mixed)
        grad_mixed = split(grad_mixed)
        buf[c, :, 0:qkv] += product(fo, grad_mixed, 0, 0)
        mid[i] += product(grad_mixed, weight(c, 0, qkv), 1, 1)

        @pl.when(c == 1)
        def _():
            first, first_inverse = normalize(xs[i])
            grad_first = mid[i]
            small_grads[0, 0:1, 0:width] += total(grad_first * first)
            small_grads[0, 1:2, 0:width] += total(grad_first)
            xs[i] = back[i] + norm_back(grad_first, first, first_inverse, vec(0))
            keep, give, _ = image_copies(1, xs, gx_ref, i)
            keep.start()
            give.start()

        return 0

    lax.fori_loop(0, 2 * own, attend_back, 0)

    for c in range(2):
        bias = sum(moved(small_grads[c, 6:7, t * LANES:(t + 1) * LANES], attention_bias_at(t), 1) for t in range(5))
        hidden = [sum(moved(small_grads[c, 7:8, t * LANES:(t + 1) * LANES], hidden_bias_at(half, t), 1)
                      for t in range(hidden_local // LANES)) for half in range(2)]
        six = small_grads[0, 0:6, 0:width]
        packed = jnp.concatenate([six, bias, hidden[0], hidden[1], jnp.zeros((LANES - 9, width), f32)], axis=0)
        buf[c, :, small:up] = packed.T
    scatter_start(0)
    for slab in back_order:
        if slab == back_order[-first_size]:
            scatter_event(1, back_order[-1])
        scatter_event(0, slab)
    for t, source, ref in ((0, yb, y_ref), (1, xs, gx_ref)):
        for i in range(own):
            keep, give, take = image_copies(t, source, ref, i)
            keep.wait()
            give.wait_send()
            take.wait_recv()
    scatter_end(1)
    scatter_end(0)


def run_step(mixer, turned, small, up, down, inputs, cotangent, n, heads, head, length):
    sizes = rings(n)
    width = inputs.shape[1]
    images = inputs.shape[0] // length
    own = images // 2
    rows = -(-length // 16) * 16
    share, hidden_local = up.shape
    columns = 7 * LANES + 2 * hidden_local
    anywhere = pl.BlockSpec(memory_space=pl.ANY)
    act = pltpu.VMEM((own, rows, width), bf16)
    full = pltpu.VMEM((own, rows, width), f32)
    dma = pltpu.SemaphoreType.DMA
    probs = pltpu.VMEM((own, 2, heads, rows, rows), bf16)
    return pl.pallas_call(
        functools.partial(step_kernel, sizes, length, heads, head),
        out_shape=[jax.ShapeDtypeStruct((share, columns), f32), jax.ShapeDtypeStruct((images, rows, width), f32),
                   jax.ShapeDtypeStruct((images, rows, width), f32)],
        in_specs=[pl.BlockSpec(memory_space=pltpu.VMEM)] * 5 + [anywhere] * 2,
        out_specs=[pl.BlockSpec(memory_space=pltpu.VMEM), anywhere, anywhere],
        scratch_shapes=[
            pltpu.VMEM((share, columns), f32),
            pltpu.VMEM((2, width, columns), f32),
            pltpu.VMEM((2, width, columns), bf16), pltpu.VMEM((2, width, columns), bf16),
            full, full, act, act, act, act, act, act, act, act,
            pltpu.VMEM((own, 2, rows, 5 * LANES), f32), probs, probs,
            pltpu.VMEM((own, 2, rows, 2 * LANES), f32), full, full, full,
            pltpu.VMEM((width // LANES, inputs.shape[0], LANES), f32),
            pltpu.VMEM((8, width), f32), pltpu.VMEM((2, 1, 5 * LANES), f32), pltpu.VMEM((2, 1, hidden_local), f32),
            pltpu.VMEM((2, 8, hidden_local), f32),
            pltpu.VMEM((n, share, columns), f32), pltpu.VMEM((n - 1, share, columns), f32),
            dma((2, 3, n)), dma((2, n)), dma((2, n)), dma((2, n)),
            dma((2, n)), dma((2, n)), dma((2, n)), dma((2, n)),
            dma((width // LANES,)), dma((2, own)), dma((2, own)), dma((2, own)),
        ],
        compiler_params=pltpu.CompilerParams(
            collective_id=2, has_side_effects=True, vmem_limit_bytes=67043328),
        name="step",
    )(mixer, turned, small, up, down, inputs, cotangent)


def pack_attention(mixer, output):
    head = mixer.shape[2] // 3
    pair = 2 * head
    out = output.T
    q, k, v = mixer[:, 0], mixer[:, 1], mixer[:, 2]
    return jnp.concatenate([q[:, :pair], k[:, :pair], v[:, :pair], q[:, pair:], k[:, pair:], v[:, pair:],
                            out[:, pair:], out[:, :pair]], axis=1)


def unpack_attention(block, head):
    pair = 2 * head
    cut = [block[:, t * head:(t + 1) * head] for t in range(12)]
    mixer = jnp.stack([jnp.concatenate(t, axis=1) for t in (
        (cut[0], cut[1], cut[6]), (cut[2], cut[3], cut[7]), (cut[4], cut[5], cut[8]))], axis=1)
    output = jnp.concatenate([cut[10], cut[11], cut[9]], axis=1).T
    return mixer, output


SMALL = ("first_gain", "first_shift", "output_bias", "second_gain", "second_shift", "reduce_bias",
         "mixer_bias", "expand_bias")


def pack_small(values):
    return jnp.concatenate([values[name].reshape(-1) for name in SMALL])


def unpack_small(flat, like):
    out, start = {}, 0
    for name in SMALL:
        size = like[name].size
        out[name] = flat[start:start + size].reshape(like[name].shape)
        start += size
    return out


def adam_update(param, grad, momentum, variance, decay):
    momentum_next = beta_one * momentum + (1.0 - beta_one) * grad
    variance_next = beta_two * variance + (1.0 - beta_two) * grad * grad
    mean_hat = momentum_next / (1.0 - beta_one**step_count)
    square_hat = variance_next / (1.0 - beta_two**step_count)
    stepped = param - learn_rate * (mean_hat / (jnp.sqrt(square_hat) + adam_eps) + decay * param)
    return (stepped, momentum_next, variance_next)


NAMES = ("first_gain", "first_shift", "mixer_weight", "mixer_bias", "output_weight", "output_bias", "second_gain",
         "second_shift", "expand_weight", "expand_bias", "reduce_weight", "reduce_bias")
DECAYED = ("mixer_weight", "output_weight", "expand_weight", "reduce_weight")


def per_device(inputs, cotangent, *rest):
    if rest[0].shape[0] % 8 == 0:
        return one_kernel(inputs, cotangent, *rest)
    return three_kernels(inputs, cotangent, *rest)


def finish(params, momenta, variances, gradients, block_out, input_gradient):
    results = [adam_update(params[m], gradients[m], momenta[m], variances[m], weight_decay if m in DECAYED else 0.0)
               for m in NAMES]
    return (block_out, input_gradient, *(gradients[m] for m in NAMES), *(r[0] for r in results),
            *(r[1] for r in results), *(r[2] for r in results))


def one_kernel(inputs, cotangent, *rest):
    n = lax.axis_size("dp")
    images, length, width = inputs.shape
    scale = (n * images * length) ** (-0.5)
    params = dict(zip(NAMES, rest[:12]))
    momenta = dict(zip(NAMES, rest[12:24]))
    variances = dict(zip(NAMES, rest[24:]))
    share = params["first_gain"].shape[0]
    heads, piece = params["mixer_bias"].shape[1:]
    head = piece * n
    hidden_local = params["expand_weight"].shape[1]
    small = jnp.pad(pack_small(params).reshape(-1, share).T, ((0, 0), (0, LANES - 9)))
    def tokens(v):
        return v.transpose(1, 0, 2).reshape(length * images, width)

    summed, block_out, input_gradient = run_step(
        params["mixer_weight"].transpose(1, 0, 2), params["output_weight"].T, small, params["expand_weight"],
        params["reduce_weight"].T, tokens(inputs), tokens(cotangent), n, heads, head, length)
    summed = summed * scale
    mixer, output = unpack_attention(summed[:, :6 * LANES], head)
    gradients = unpack_small(summed[:, 6 * LANES:6 * LANES + 9].T.reshape(-1), params)
    up = 7 * LANES
    gradients.update(mixer_weight=mixer, output_weight=output, expand_weight=summed[:, up:up + hidden_local],
                     reduce_weight=summed[:, up + hidden_local:].T)
    return finish(params, momenta, variances, gradients, block_out[:, :length], input_gradient[:, :length])


def three_kernels(inputs, cotangent, *rest):
    n = lax.axis_size("dp")
    scale = (n * inputs.shape[0] * inputs.shape[1]) ** (-0.5)
    params = dict(zip(NAMES, rest[:12]))
    momenta = dict(zip(NAMES, rest[12:24]))
    variances = dict(zip(NAMES, rest[24:]))
    share, width = params["first_gain"].shape[0], inputs.shape[2]
    heads, piece = params["mixer_bias"].shape[1:]
    head = piece * n
    hidden_local = params["expand_weight"].shape[1]
    end = 6 * LANES + 2 * hidden_local

    small = pack_small(params)
    count = small.shape[0]
    slab = jnp.concatenate([
        pack_attention(params["mixer_weight"], params["output_weight"]),
        params["expand_weight"], params["reduce_weight"].T,
        jnp.pad(small, (0, share * LANES - count)).reshape(share, LANES)], axis=1)
    columns = slab.shape[1]
    gathered = gather(slab, n)

    flat = gathered[:, :, :, end:].reshape(2, n, share * LANES)[:, :, :count]
    vectors = jnp.pad(flat[0, :, :6 * share].reshape(n, 6, share).transpose(1, 0, 2).reshape(6, width),
                      ((0, 2), (0, 0)))
    bias = flat[:, :, 6 * share:7 * share].reshape(2, n, 2, heads, piece).transpose(0, 2, 3, 1, 4)
    bias = bias.reshape(2, 2, heads * head)
    q, v, none = bias[:, 0], bias[:, 1], jnp.zeros((2, 2 * head), f32)
    mixed_bias = jnp.concatenate([q[:, :2 * head], none, v[:, :2 * head], q[:, 2 * head:], none[:, :head],
                                  v[:, 2 * head:], none[:, :head]], axis=1)[:, None]
    expand_bias = flat[:, :, 7 * share:].reshape(2, n, -1, piece).transpose(0, 2, 1, 3).reshape(2, 1, -1)

    base = (lax.axis_index("mp") * (inputs.shape[0] // 2)).astype(jnp.int32).reshape(1)
    block_out, input_gradient, grads, small_grads = run_layer(
        base, inputs, cotangent, gathered.reshape(2, width, columns), vectors, mixed_bias, expand_bias, heads, head)

    total = small_grads[:1, :6, :width].reshape(6, n, share).transpose(1, 0, 2).reshape(n, 6 * share)
    row = small_grads[:, 6, :5 * LANES]
    bias = jnp.stack([
        jnp.concatenate([row[:, :2 * head], row[:, 6 * head:7 * head]], axis=1),
        jnp.concatenate([row[:, 4 * head:6 * head], row[:, 8 * head:9 * head]], axis=1)], axis=1)
    bias = bias.reshape(2, 2, heads, n, piece).transpose(0, 3, 1, 2, 4).reshape(2, n, share)
    hidden = small_grads[:, 7].reshape(2, hidden_local // head, n, piece).transpose(0, 2, 1, 3).reshape(2, n, -1)
    packed = jnp.concatenate([jnp.broadcast_to(total[None], (2,) + total.shape), bias, hidden], axis=2)
    packed = jnp.pad(packed, ((0, 0), (0, 0), (0, share * LANES - count))).reshape(2, n, share, LANES)
    grads = lax.dynamic_update_slice(grads.reshape(2, n, share, columns), packed, (0, 0, 0, end))

    summed, block_out, input_gradient = scatter(grads, block_out, input_gradient, n)
    summed = summed * scale
    mixer, output = unpack_attention(summed[:, :6 * LANES], head)
    gradients = unpack_small(summed[:, end:].reshape(-1), params)
    gradients.update(mixer_weight=mixer, output_weight=output,
                     expand_weight=summed[:, 6 * LANES:6 * LANES + hidden_local],
                     reduce_weight=summed[:, 6 * LANES + hidden_local:end].T)
    return finish(params, momenta, variances, gradients, block_out, input_gradient)


def solution(mesh):
    images = P("dp", None, None)
    entries = (P("dp"), P("dp"), P("dp", None, "mp"), P(None, "mp", "dp"), P("mp", "dp"), P("dp"), P("dp"), P("dp"),
               P("dp", "mp"), P("mp", "dp"), P("mp", "dp"), P("dp"))
    return jax.shard_map(per_device, mesh=mesh, in_specs=(images, images) + entries * 3,
                         out_specs=(images, images) + entries * 4, check_vma=False)
```

```python
import functools
import heapq

import jax
import jax.numpy as jnp
from jax import lax
from jax.experimental import pallas as pl
from jax.experimental.pallas import tpu as pltpu
from jax.sharding import PartitionSpec as P

norm_eps = 1e-06
beta_one = 0.9
beta_two = 0.99
adam_eps = 1e-08
learn_rate = 0.05
weight_decay = 0.05
step_count = 3.0

LANES = 128
MASKED = -1e30
f32, bf16 = jnp.float32, jnp.bfloat16


def split(x):
    high = x.astype(bf16)
    return high, (x - high.astype(f32)).astype(bf16)


def dot(a, b, da, db):
    return lax.dot_general(a, b, (((da,), (db,)), ((), ())), preferred_element_type=f32)


def product(a, b, da, db):
    left = jnp.concatenate([a[0], a[0], a[1]], axis=da)
    right = jnp.concatenate([b[0], b[1], b[0]], axis=db)
    return dot(left, right, da, db)


def product_apart(a, b, da, db):
    n = b[0].shape[1 - db]
    both = dot(a[0], jnp.concatenate(b, axis=1 - db), da, db)
    return both[:, :n] + both[:, n:] + dot(a[1], b[0], da, db)


def layer_kernel(length, heads, head, base, x_ref, cot_ref, w_ref, vec_ref, mb_ref, eb_ref,
                 y_ref, gx_ref, g_ref, sg_ref,
                 whi, wlo, wsem, pad, mixed, probs_hi, probs_lo, joined,
                 fo_hi, fo_lo, so_hi, so_lo, cot_hi, cot_lo, gm_hi, gm_lo, part, part2):
    step = pl.program_id(0)
    rows, width = pad.shape[1], pad.shape[2]
    local = heads * head
    qkv = 5 * LANES
    hidden_local = eb_ref.shape[-1]
    attn = 6 * LANES
    up, down, end = attn, attn + hidden_local, attn + 2 * hidden_local

    @pl.when(step == 0)
    def _():
        for c in range(2):
            pltpu.make_async_copy(w_ref.at[c], g_ref.at[c], wsem.at[c]).start()
        pad[...] = jnp.zeros_like(pad)
        sg_ref[...] = jnp.zeros_like(sg_ref)
        for c in range(2):
            pltpu.make_async_copy(w_ref.at[c], g_ref.at[c], wsem.at[c]).wait()

        def convert(t, _):
            c, r = t // (width // 16), t % (width // 16)
            at = pl.ds(pl.multiple_of(r * 16, 16), 16)
            high, low = split(g_ref[c, at, 0:end])
            whi[c, at, :] = high
            wlo[c, at, :] = low
            g_ref[c, at, :] = jnp.zeros((16, g_ref.shape[2]), f32)
            return 0

        lax.fori_loop(0, 2 * (width // 16), convert, 0)

    def weight(c, lo, hi):
        return whi[c, :, lo:hi], wlo[c, :, lo:hi]

    def vec(r):
        return vec_ref[r:r + 1, :]

    def normalize(v):
        center = v - jnp.mean(v, axis=-1, keepdims=True)
        inverse = lax.rsqrt(jnp.mean(center * center, axis=-1, keepdims=True) + norm_eps)
        return center * inverse, inverse

    def norm_back(grad, normed, inverse, gain):
        scaled = grad * gain
        return inverse * (scaled - jnp.mean(scaled, axis=-1, keepdims=True)
                          - normed * jnp.mean(scaled * normed, axis=-1, keepdims=True))

    def total(v):
        return jnp.sum(v, axis=0, keepdims=True)

    pad[0, 0:length, :] = x_ref[0]
    pad[1, 0:length, :] = cot_ref[0]
    x, cot = pad[0], pad[1]
    cot_hi[...], cot_lo[...] = split(cot)
    first, first_inverse = normalize(x)
    fo_hi[...], fo_lo[...] = split(first * vec(0) + vec(1))

    lane = lax.broadcasted_iota(jnp.int32, (rows, LANES), 1)
    sides = (lane < head, lane >= head)
    column = lax.broadcasted_iota(jnp.int32, (rows, rows), 1)
    score_scale = head ** (-0.5)

    def side(v, s):
        return jnp.where(sides[s], v, 0.0)

    def swap(v):
        return pltpu.roll(v, head, 1)

    def windows(c):
        w = [mixed[c, :, t * LANES:(t + 1) * LANES] for t in range(5)]
        third = side(w[3], 0) * score_scale, side(swap(w[3]), 0), side(w[4], 0)
        return [
            (side(w[0], 0) * score_scale, side(w[1], 0), side(w[2], 0)),
            (side(w[0], 1) * score_scale, side(w[1], 1), side(w[2], 1)),
            third,
        ]

    part[...] = jnp.zeros_like(part)

    def attend(c, _):
        mixed[c] = product((fo_hi[...], fo_lo[...]), weight(c, 0, qkv), 1, 0) + mb_ref[c]
        outs = []
        for h, (q, k, v) in enumerate(windows(c)):
            scores = product(split(q), split(k), 1, 1)
            scores = jnp.where(column < length, scores, MASKED)
            expon = jnp.exp(scores - jnp.max(scores, axis=-1, keepdims=True))
            probs = split(expon / jnp.sum(expon, axis=-1, keepdims=True))
            probs_hi[c, h], probs_lo[c, h] = probs
            outs.append(product_apart(probs, split(v), 1, 0))
        joined[c] = jnp.concatenate([swap(outs[2]), outs[0] + outs[1]], axis=1)
        part[...] += product(split(joined[c]), weight(c, 4 * LANES, attn), 1, 1)
        return 0

    lax.fori_loop(0, 2, attend, 0)
    middle = x + part[...] + vec(2)
    second, second_inverse = normalize(middle)
    so_hi[...], so_lo[...] = split(second * vec(3) + vec(4))

    part[...] = middle + vec(5)
    part2[...] = jnp.zeros_like(part2)

    def feed(c, _):
        so = (so_hi[...], so_lo[...])
        co = (cot_hi[...], cot_lo[...])
        hidden = product(so, weight(c, up, down), 1, 0) + eb_ref[c]
        share = 0.5 * (1.0 + lax.erf(hidden * (0.5 ** 0.5)))
        active = split(hidden * share)
        slope = share + hidden * jnp.exp(-0.5 * hidden * hidden) * 0.3989422804014327
        part[...] += product(active, weight(c, down, end), 1, 1)
        g_ref[c, :, down:end] += product(co, active, 0, 0)
        grad = product(co, weight(c, down, end), 1, 0) * slope
        sg_ref[c, 7:8, 0:hidden_local] += total(grad)
        grad = split(grad)
        g_ref[c, :, up:down] += product(so, grad, 0, 0)
        part2[...] += product(grad, weight(c, up, down), 1, 1)
        return 0

    lax.fori_loop(0, 2, feed, 0)
    y_ref[0] = part[0:length, :]

    grad_second = part2[...]
    sg_ref[0, 3:4, 0:width] += total(grad_second * second)
    sg_ref[0, 4:5, 0:width] += total(grad_second)
    sg_ref[0, 5:6, 0:width] += total(cot)
    grad_middle = cot + norm_back(grad_second, second, second_inverse, vec(3))
    sg_ref[0, 2:3, 0:width] += total(grad_middle)
    gm_hi[...], gm_lo[...] = split(grad_middle)
    part2[...] = grad_middle

    part[...] = jnp.zeros_like(part)

    def attend_back(c, _):
        gm = (gm_hi[...], gm_lo[...])
        fo = (fo_hi[...], fo_lo[...])
        grad_heads = product(gm, weight(c, 4 * LANES, attn), 1, 0)
        g_ref[c, :, 4 * LANES:attn] += product(gm, split(joined[c]), 0, 0)
        pair, single = grad_heads[:, LANES:], swap(grad_heads[:, :LANES])
        pair_out, single_out = joined[c, :, LANES:], swap(joined[c, :, :LANES])
        grad_outs = (side(pair, 0), side(pair, 1), side(single, 0))
        outs = (pair_out, pair_out, single_out)
        grads = []
        for h, (q, k, v) in enumerate(windows(c)):
            grad_out = grad_outs[h]
            row = jnp.sum(grad_out * outs[h], axis=-1, keepdims=True)
            grad_out = split(grad_out)
            grad_probs = product(grad_out, split(v), 1, 1)
            probs = (probs_hi[c, h], probs_lo[c, h])
            grad_v = product_apart(probs, grad_out, 0, 0)
            grad_scores = split((probs[0].astype(f32) + probs[1].astype(f32)) * (grad_probs - row))
            grad_q = product_apart(grad_scores, split(k), 1, 0) * score_scale
            grad_k = product_apart(grad_scores, split(q), 0, 0)
            grads.append((grad_q, grad_k, grad_v))
        one, two, three = grads
        grad_mixed = jnp.concatenate(
            [one[0] + two[0], one[1] + two[1], one[2] + two[2], three[0] + swap(three[1]), three[2]], axis=1)
        sg_ref[c, 6:7, 0:qkv] += total(grad_mixed)
        grad_mixed = split(grad_mixed)
        g_ref[c, :, 0:qkv] += product(fo, grad_mixed, 0, 0)
        part[...] += product(grad_mixed, weight(c, 0, qkv), 1, 1)
        return 0

    lax.fori_loop(0, 2, attend_back, 0)
    grad_first = part[...]
    sg_ref[0, 0:1, 0:width] += total(grad_first * first)
    sg_ref[0, 1:2, 0:width] += total(grad_first)
    gx_ref[0] = (part2[...] + norm_back(grad_first, first, first_inverse, vec(0)))[0:length, :]


def run_layer(base, inputs, cotangent, weights, vectors, mixed_bias, expand_bias, heads, head):
    images, length, width = inputs.shape
    own = images // 2
    rows = -(-length // 16) * 16
    columns = weights.shape[-1]
    hidden_local = expand_bias.shape[-1]
    end = 6 * LANES + 2 * hidden_local
    image = pl.BlockSpec((1, length, width), lambda i, b: (b[0] + i, 0, 0))

    def whole(shape):
        return pl.BlockSpec(shape, lambda i, b: (0,) * len(shape))

    act = pltpu.VMEM((rows, width), bf16)
    return pl.pallas_call(
        functools.partial(layer_kernel, length, heads, head),
        grid_spec=pltpu.PrefetchScalarGridSpec(
            num_scalar_prefetch=1,
            grid=(own,),
            in_specs=[image, image, pl.BlockSpec(memory_space=pl.ANY), whole(vectors.shape),
                      whole(mixed_bias.shape), whole(expand_bias.shape)],
            out_specs=[image, image, whole((2, width, columns)), whole((2, 8, hidden_local))],
            scratch_shapes=[
                pltpu.VMEM((2, width, end), bf16), pltpu.VMEM((2, width, end), bf16),
                pltpu.SemaphoreType.DMA((2,)),
                pltpu.VMEM((2, rows, width), f32),
                pltpu.VMEM((2, rows, 5 * LANES), f32),
                pltpu.VMEM((2, heads, rows, rows), bf16), pltpu.VMEM((2, heads, rows, rows), bf16),
                pltpu.VMEM((2, rows, 2 * LANES), f32),
                act, act, act, act, act, act, act, act,
                pltpu.VMEM((rows, width), f32), pltpu.VMEM((rows, width), f32),
            ],
        ),
        out_shape=[
            jax.ShapeDtypeStruct(inputs.shape, f32), jax.ShapeDtypeStruct(inputs.shape, f32),
            jax.ShapeDtypeStruct((2, width, columns), f32), jax.ShapeDtypeStruct((2, 8, hidden_local), f32),
        ],
        compiler_params=pltpu.CompilerParams(
            dimension_semantics=("arbitrary",), vmem_limit_bytes=60 * 2**20),
        name="layer",
    )(base, inputs, cotangent, weights, vectors, mixed_bias, expand_bias)


def rings(n):
    side = max(k for k in range(1, n + 1) if n % (k * k) == 0 and n // (k * k) >= k)
    return n // (side * side), side, side


def place(sizes):
    first, side, _ = sizes
    core, me = lax.axis_index("mp"), lax.axis_index("dp")
    a, b, c = lax.div(me, side * side), lax.rem(lax.div(me, side), side), lax.rem(me, side)
    firsts = [lax.rem(a + i, first) * (side * side) for i in range(first)]
    bs = [lax.rem(b + j, side) for j in range(side)]
    cs = [lax.rem(c + j, side) for j in range(side)]
    cores = {"mine": core, "other": 1 - core}
    pairs = {}
    for of, which in cores.items():
        for j in range(side):
            for k in range(side):
                ahead_b = bs[j] * which + bs[k] * (1 - which)
                ahead_c = cs[k] * which + cs[j] * (1 - which)
                pairs[of, j, k] = ahead_b * side + ahead_c
    places = {(of, i, j, k): firsts[i] + pairs[of, j, k]
              for of in cores for i in range(first) for j in range(side) for k in range(side)}

    def at(slab, sign=1, of="mine"):
        i, j, k = slab
        return places[of, (sign * i) % first, (sign * j) % side, (sign * k) % side]

    return core, at


UNITS = ((1, 0, 0), (0, 1, 0), (0, 0, 1))


def plus(slab, unit):
    return tuple(s + u for s, u in zip(slab, unit))


def sends(slab, sizes):
    out = [(0, (i, 0, 0), (i, 0, 0)) for i in range(1, sizes[0])] if not any(slab) else []
    for r in (1, 2):
        if not any(slab[r + 1:]) and slab[r] + 1 < sizes[r]:
            out.append((r, UNITS[r], plus(slab, UNITS[r])))
    return out


def sources(slab, sizes):
    out = [(i, 0, 0) for i in range(1, sizes[0])] if not any(slab) else []
    for r in (1, 2):
        if not any(slab[r + 1:]) and slab[r] + 1 < sizes[r]:
            out.append(plus(slab, UNITS[r]))
    return out


def hop(slab):
    r = max(q for q in range(3) if slab[q])
    return slab if r == 0 else UNITS[r]


def arrival_order(sizes):
    cost, free, heap, order = (2.0, 1.5, 1.5), [0.0] * 3, [(0.0, (0, 0, 0))], []
    while heap:
        now, slab = heapq.heappop(heap)
        order.append(slab)
        for r, _, there in sends(slab, sizes):
            free[r] = max(now, free[r]) + cost[r]
            heapq.heappush(heap, (free[r] + 1.0, there))
    return order


def slab_id(slab, sizes):
    return (slab[0] * sizes[1] + slab[1]) * sizes[2] + slab[2]


def greet(core, at, sizes):
    barrier = pltpu.get_barrier_semaphore()
    backs = [(i, 0, 0) for i in range(1, sizes[0])] + [UNITS[1], UNITS[2]]
    for steps in backs:
        pl.semaphore_signal(barrier, inc=1, device_id={"dp": at(steps, -1)})
    pl.semaphore_signal(barrier, inc=1, device_id={"mp": 1 - core})
    pl.semaphore_wait(barrier, len(backs) + 1)


def gather_kernel(sizes, slab_ref, out_ref, send_sem, recv_sem, swap_send, swap_recv, own_sem):
    core, at = place(sizes)
    number = functools.partial(slab_id, sizes=sizes)
    greet(core, at, sizes)

    def landing(slab, of):
        return out_ref.at[core if of == "mine" else 1 - core, at(slab, -1, of)]

    started = []
    own = pltpu.make_async_copy(slab_ref, landing((0, 0, 0), "mine"), own_sem)
    for slab in arrival_order(sizes):
        spot = landing(slab, "mine")
        if any(slab):
            pltpu.make_async_remote_copy(
                src_ref=spot, dst_ref=spot, send_sem=send_sem.at[0, 0], recv_sem=recv_sem.at[number(slab)],
                device_id={"mp": 1 - core}).wait_recv()
        source = spot if any(slab) else slab_ref
        for r, steps, there in reversed(sends(slab, sizes)):
            copy = pltpu.make_async_remote_copy(
                src_ref=source, dst_ref=spot, send_sem=send_sem.at[r, number(there)],
                recv_sem=recv_sem.at[number(there)], device_id={"dp": at(steps)})
            copy.start()
            started.append(copy)
        copy = pltpu.make_async_remote_copy(
            src_ref=source, dst_ref=spot, send_sem=swap_send.at[number(slab)], recv_sem=swap_recv.at[number(slab)],
            device_id={"mp": 1 - core})
        copy.start()
        started.append(copy)
        if not any(slab):
            own.start()
    for slab in arrival_order(sizes):
        spot = landing(slab, "other")
        pltpu.make_async_remote_copy(
            src_ref=spot, dst_ref=spot, send_sem=swap_send.at[0], recv_sem=swap_recv.at[number(slab)],
            device_id={"mp": 1 - core}).wait_recv()
    for copy in started:
        copy.wait_send()
    own.wait()


def gather(slab, n):
    sizes = rings(n)
    return pl.pallas_call(
        functools.partial(gather_kernel, sizes),
        out_shape=jax.ShapeDtypeStruct((2, n) + slab.shape, f32),
        in_specs=[pl.BlockSpec(memory_space=pltpu.VMEM)],
        out_specs=pl.BlockSpec(memory_space=pl.ANY),
        scratch_shapes=[
            pltpu.SemaphoreType.DMA((3, n)), pltpu.SemaphoreType.DMA((n,)),
            pltpu.SemaphoreType.DMA((n,)), pltpu.SemaphoreType.DMA((n,)), pltpu.SemaphoreType.DMA,
        ],
        compiler_params=pltpu.CompilerParams(collective_id=0, has_side_effects=True),
        name="gather",
    )(slab)


def scatter_kernel(sizes, g_ref, y_in, gx_in, out_ref, y_ref, gx_ref,
                   acc, swapped, landed, load_sem, send_sem, recv_sem, swap_send, swap_recv, image_send, image_recv):
    del y_in, gx_in
    core, at = place(sizes)
    number = functools.partial(slab_id, sizes=sizes)
    greet(core, at, sizes)
    first, side, _ = sizes
    order = [(i, j, k) for k in reversed(range(side)) for j in reversed(range(side)) for i in reversed(range(first))]
    own = y_ref.shape[0] // 2
    started, loads, images = [], {}, []
    for slab in order:
        s = number(slab)
        copy = pltpu.make_async_remote_copy(
            src_ref=g_ref.at[1 - core, at(slab, 1, "other")], dst_ref=swapped.at[s],
            send_sem=swap_send.at[s], recv_sem=swap_recv.at[s], device_id={"mp": 1 - core})
        copy.start()
        started.append(copy)
        loads[slab] = pltpu.make_async_copy(g_ref.at[core, at(slab)], acc.at[s], load_sem.at[s])
        loads[slab].start()
    for t, ref in enumerate((y_ref, gx_ref)):
        mine = ref.at[pl.ds(core * own, own)]
        copy = pltpu.make_async_remote_copy(
            src_ref=mine, dst_ref=mine, send_sem=image_send.at[t], recv_sem=image_recv.at[t],
            device_id={"mp": 1 - core})
        copy.start()
        started.append(copy)
        theirs = ref.at[pl.ds((1 - core) * own, own)]
        images.append(pltpu.make_async_remote_copy(
            src_ref=theirs, dst_ref=theirs, send_sem=image_send.at[t], recv_sem=image_recv.at[t],
            device_id={"mp": 1 - core}))

    def arrived(buffer, spot, sem):
        pltpu.make_async_remote_copy(
            src_ref=buffer.at[spot], dst_ref=buffer.at[spot], send_sem=swap_send.at[0], recv_sem=sem,
            device_id={"mp": 1 - core}).wait_recv()
        return buffer[spot]

    for slab in order:
        s = number(slab)
        loads[slab].wait()
        value = acc[s] + arrived(swapped, s, swap_recv.at[s])
        for other in sources(slab, sizes):
            spot = number(other)
            value = value + arrived(landed, spot - 1, recv_sem.at[spot])
        if any(slab):
            acc[s] = value
            copy = pltpu.make_async_remote_copy(
                src_ref=acc.at[s], dst_ref=landed.at[s - 1], send_sem=send_sem.at[s], recv_sem=recv_sem.at[s],
                device_id={"dp": at(hop(slab))})
            copy.start()
            started.append(copy)
        else:
            out_ref[...] = value
    for copy in images:
        copy.wait_recv()
    for copy in started:
        copy.wait_send()


def scatter(grads, block_out, input_gradient, n):
    sizes = rings(n)
    slab = grads.shape[2:]
    anywhere = pl.BlockSpec(memory_space=pl.ANY)
    return pl.pallas_call(
        functools.partial(scatter_kernel, sizes),
        out_shape=[jax.ShapeDtypeStruct(slab, f32), jax.ShapeDtypeStruct(block_out.shape, f32),
                   jax.ShapeDtypeStruct(input_gradient.shape, f32)],
        in_specs=[anywhere] * 3,
        out_specs=[pl.BlockSpec(memory_space=pltpu.VMEM), anywhere, anywhere],
        input_output_aliases={1: 1, 2: 2},
        scratch_shapes=[
            pltpu.VMEM((n,) + slab, f32), pltpu.VMEM((n,) + slab, f32), pltpu.VMEM((n - 1,) + slab, f32),
            pltpu.SemaphoreType.DMA((n,)), pltpu.SemaphoreType.DMA((n,)), pltpu.SemaphoreType.DMA((n,)),
            pltpu.SemaphoreType.DMA((n,)), pltpu.SemaphoreType.DMA((n,)),
            pltpu.SemaphoreType.DMA((2,)), pltpu.SemaphoreType.DMA((2,)),
        ],
        compiler_params=pltpu.CompilerParams(
            collective_id=1, has_side_effects=True, vmem_limit_bytes=60 * 2**20),
        name="scatter",
    )(grads, block_out, input_gradient)


def spread(count, slots, lead):
    return [min(slots - 1, lead + (e * (slots - lead)) // count) for e in range(count)]


def step_kernel(sizes, length, heads, head, mixer_ref, turned_ref, small_ref, up_ref, down_ref, x_ref, cot_ref, out_ref, y_ref, gx_ref,
                slab_ref, buf, whi, wlo, xs, cots, fo_hi, fo_lo, so_hi, so_lo, cot_hi, cot_lo, gm_hi, gm_lo,
                mixed, probs_hi, probs_lo, joined, mid, back, yb, staged, vec_ref, bias_ref, hidden_bias, small_grads, mixed_hot, hidden_hot,
                swapped, landed, send_sem, recv_sem, swap_send, swap_recv,
                push_send, push_recv, trade_send, trade_recv, stage_sem, image_sem, image_send, image_recv):
    core, at = place(sizes)
    number = functools.partial(slab_id, sizes=sizes)
    n = sizes[0] * sizes[1] * sizes[2]
    own, rows, width = xs.shape
    share = up_ref.shape[0]
    hidden_local = hidden_bias.shape[-1]
    qkv, attn = 5 * LANES, 6 * LANES
    small, up = attn, attn + LANES
    down, end = up + hidden_local, up + 2 * hidden_local
    spans = ((0, up), (up, end))
    partner = {"mp": 1 - core}

    def block(slab, sign, of):
        return pl.ds(pl.multiple_of(at(slab, sign, of) * share, 8), share)

    def span(p):
        return slice(*spans[p])

    def landing(p, slab, of):
        return buf.at[core if of == "mine" else 1 - core, block(slab, -1, of), span(p)]

    def gather_event(p, slab, along=(0, 1, 2), swap=True):
        spot = landing(p, slab, "mine")
        if any(slab):
            pltpu.make_async_remote_copy(
                src_ref=spot, dst_ref=spot, send_sem=send_sem.at[p, 0, 0], recv_sem=recv_sem.at[p, number(slab)],
                device_id=partner).wait_recv()
        source = spot if any(slab) else slab_ref.at[:, span(p)]
        for r, steps, there in reversed(sends(slab, sizes)):
            if r in along:
                pltpu.make_async_remote_copy(
                    src_ref=source, dst_ref=spot, send_sem=send_sem.at[p, r, number(there)],
                    recv_sem=recv_sem.at[p, number(there)], device_id={"dp": at(steps)}).start()
        if swap:
            pltpu.make_async_remote_copy(
                src_ref=source, dst_ref=spot, send_sem=swap_send.at[p, number(slab)],
                recv_sem=swap_recv.at[p, number(slab)], device_id=partner).start()

    def gather_end(p):
        for slab in order:
            spot = landing(p, slab, "other")
            pltpu.make_async_remote_copy(
                src_ref=spot, dst_ref=spot, send_sem=swap_send.at[p, 0], recv_sem=swap_recv.at[p, number(slab)],
                device_id=partner).wait_recv()
        for slab in order:
            spot = landing(p, slab, "mine")
            for r, _, there in sends(slab, sizes):
                pltpu.make_async_remote_copy(
                    src_ref=spot, dst_ref=spot, send_sem=send_sem.at[p, r, number(there)],
                    recv_sem=recv_sem.at[p, 0], device_id=partner).wait_send()
            pltpu.make_async_remote_copy(
                src_ref=spot, dst_ref=spot, send_sem=swap_send.at[p, number(slab)], recv_sem=swap_recv.at[p, 0],
                device_id=partner).wait_send()

    order = arrival_order(sizes)

    first_size, side_size, _ = sizes
    back_order = [(i, j, k) for k in reversed(range(side_size)) for j in reversed(range(side_size))
                  for i in reversed(range(first_size))]

    def trade(p, slab):
        s = number(slab)
        return pltpu.make_async_remote_copy(
            src_ref=buf.at[1 - core, block(slab, 1, "other"), span(p)], dst_ref=swapped.at[s, :, span(p)],
            send_sem=trade_send.at[p, s], recv_sem=trade_recv.at[p, s], device_id=partner)

    def scatter_start(p):
        for slab in back_order:
            trade(p, slab).start()

    def arrived(buffer, spot, p, sem):
        ref = buffer.at[spot, :, span(p)]
        pltpu.make_async_remote_copy(
            src_ref=ref, dst_ref=ref, send_sem=trade_send.at[p, 0], recv_sem=sem, device_id=partner).wait_recv()
        return ref[...]

    def push(p, slab):
        s = number(slab)
        return pltpu.make_async_remote_copy(
            src_ref=buf.at[core, block(slab, 1, "mine"), span(p)], dst_ref=landed.at[s - 1, :, span(p)],
            send_sem=push_send.at[p, s], recv_sem=push_recv.at[p, s], device_id={"dp": at(hop(slab))})

    def scatter_event(p, slab):
        s = number(slab)
        here = (core, block(slab, 1, "mine"), span(p))
        value = buf[here] + arrived(swapped, s, p, trade_recv.at[p, s])
        for other in sources(slab, sizes):
            spot = number(other)
            value = value + arrived(landed, spot - 1, p, push_recv.at[p, spot])
        if any(slab):
            buf[here] = value
            push(p, slab).start()
        else:
            out_ref[:, span(p)] = value

    def scatter_end(p):
        for slab in back_order:
            trade(p, slab).wait_send()
            if any(slab):
                push(p, slab).wait_send()

    def image_copies(t, source, ref, i):
        spot = ref.at[core * own + i]
        keep = pltpu.make_async_copy(source.at[i], spot, image_sem.at[t, i])
        give = pltpu.make_async_remote_copy(
            src_ref=source.at[i], dst_ref=spot, send_sem=image_send.at[t, i], recv_sem=image_recv.at[t, i],
            device_id=partner)
        theirs = ref.at[(1 - core) * own + i]
        take = pltpu.make_async_remote_copy(
            src_ref=theirs, dst_ref=theirs, send_sem=image_send.at[t, i], recv_sem=image_recv.at[t, i],
            device_id=partner)
        return keep, give, take

    def weight(c, lo, hi):
        return whi[c, :, lo:hi], wlo[c, :, lo:hi]

    def vec(r):
        return vec_ref[r:r + 1, :]

    def normalize(v):
        center = v - jnp.mean(v, axis=-1, keepdims=True)
        inverse = lax.rsqrt(jnp.mean(center * center, axis=-1, keepdims=True) + norm_eps)
        return center * inverse, inverse

    def norm_back(grad, normed, inverse, gain):
        scaled = grad * gain
        return inverse * (scaled - jnp.mean(scaled, axis=-1, keepdims=True)
                          - normed * jnp.mean(scaled * normed, axis=-1, keepdims=True))

    def total(v):
        return jnp.sum(v, axis=0, keepdims=True)

    def convert(lo, hi):
        def body(t, _):
            c, r = t // (width // 16), t % (width // 16)
            here = pl.ds(pl.multiple_of(r * 16, 16), 16)
            high, low = split(buf[c, here, lo:hi])
            whi[c, here, lo:hi] = high
            wlo[c, here, lo:hi] = low
            buf[c, here, lo:hi] = jnp.zeros((16, hi - lo), f32)
            return 0

        lax.fori_loop(0, 2 * (width // 16), body, 0)

    def thirds(v):
        high = v.astype(bf16)
        v = v - high.astype(f32)
        middle_term = v.astype(bf16)
        return high, middle_term, (v - middle_term.astype(f32)).astype(bf16)

    def moved(v, onehot, dim):
        terms = jnp.concatenate([term.astype(f32) for term in thirds(v)], axis=0).astype(bf16)
        out = dot(terms, onehot, 1, dim)
        return out[4:6] + out[2:4] + out[0:2]

    piece = head // n

    def make_onehots():
        entry = lax.broadcasted_iota(jnp.int32, (width, LANES), 0)
        owner, inner = entry // share, entry % share
        target = lax.broadcasted_iota(jnp.int32, (width, LANES), 1)
        kind, which = inner // (heads * piece), (inner // piece) % heads
        window = jnp.where(kind == 0, jnp.where(which < 2, 0, 3), jnp.where(which < 2, 2, 4))
        spot = window * LANES + (which % 2) * head + owner * piece + inner % piece
        for t in range(5):
            mixed_hot[:, t * LANES:(t + 1) * LANES] = (spot == target + t * LANES).astype(f32).astype(bf16)
        for half in range(2):
            flat = inner + half * share
            spot = (flat // piece) * head + owner * piece + flat % piece
            for t in range(hidden_local // LANES):
                hidden_hot[half, :, t * LANES:(t + 1) * LANES] = (spot == target + t * LANES).astype(f32).astype(bf16)

    pair = 2 * head
    q, k, v = (mixer_ref[t] for t in range(3))
    turned = turned_ref[...]
    slab_ref[...] = jnp.concatenate(
        [q[:, :pair], k[:, :pair], v[:, :pair], q[:, pair:], k[:, pair:], v[:, pair:], turned[:, pair:], turned[:, :pair],
         small_ref[...], up_ref[...], down_ref[...]], axis=1)
    greet(core, at, sizes)
    gather_event(0, (0, 0, 0))
    gather_event(1, (0, 0, 0), (0, 1, 2))
    staging = []
    tiles = width // LANES
    for t in range(tiles):
        staging.append(pltpu.make_async_copy(x_ref.at[:, t * LANES:(t + 1) * LANES], staged.at[t], stage_sem.at[t]))
        staging[-1].start()
    buf[core, block((0, 0, 0), 1, "mine"), :] = slab_ref[...]
    xs[...] = jnp.zeros_like(xs)
    cots[...] = jnp.zeros_like(cots)
    small_grads[...] = jnp.zeros_like(small_grads)
    for source, sink in ((x_ref, xs), (cot_ref, cots)):
        for t in range(tiles):
            lanes = slice(t * LANES, (t + 1) * LANES)
            copy = pltpu.make_async_copy(source.at[:, lanes], staged.at[t], stage_sem.at[t])
            if sink is cots:
                copy.start()
            copy.wait()
            for i in range(own):
                sink[i, 0:length, lanes] = staged[t, pl.ds(core * own + i, length, stride=2 * own), :]

    make_onehots()
    for slab in order[1:]:
        gather_event(0, slab)
    for i in range(own):
        cot_hi[i], cot_lo[i] = split(cots[i])
    gather_end(0)
    turned = [buf[c, :, small:up].T[0:16] for c in range(2)]
    vec_ref[...] = turned[0][0:8, :]

    def both(r):
        return jnp.concatenate([turned[0][r:r + 1], turned[1][r:r + 1]], axis=0)

    bias = moved(both(6), mixed_hot[...], 0)
    hidden = moved(both(7), hidden_hot[0], 0) + moved(both(8), hidden_hot[1], 0)
    for c in range(2):
        bias_ref[c] = bias[c:c + 1]
        hidden_bias[c] = hidden[c:c + 1]
    convert(0, attn)

    lane = lax.broadcasted_iota(jnp.int32, (rows, LANES), 1)
    sides = (lane < head, lane >= head)
    column = lax.broadcasted_iota(jnp.int32, (rows, rows), 1)
    score_scale = head ** (-0.5)

    def side(v, s):
        return jnp.where(sides[s], v, 0.0)

    def swap(v):
        return pltpu.roll(v, head, 1)

    def windows(i, c):
        w = [mixed[i, c, :, t * LANES:(t + 1) * LANES] for t in range(5)]
        return [
            (side(w[0], 0) * score_scale, side(w[1], 0), side(w[2], 0)),
            (side(w[0], 1) * score_scale, side(w[1], 1), side(w[2], 1)),
            (side(w[3], 0) * score_scale, side(swap(w[3]), 0), side(w[4], 0)),
        ]

    def serve(t, plan, event):
        for slot in sorted({slot for slot, _ in plan}):
            @pl.when(t == slot)
            def _(slot=slot):
                for when, slab in plan:
                    if when == slot:
                        event(1, slab)

    gather_plan = list(zip(spread(len(order) - 1, 2 * own, 0), order[1:]))

    def attend(t, _):
        i, c = t // 2, t % 2

        @pl.when(c == 0)
        def _():
            normed, _ = normalize(xs[i])
            fo_hi[i], fo_lo[i] = split(normed * vec(0) + vec(1))
            mid[i] = xs[i] + vec(2)

        serve(t, gather_plan, gather_event)
        mixed[i, c] = product((fo_hi[i], fo_lo[i]), weight(c, 0, qkv), 1, 0) + bias_ref[c]
        outs = []
        for h, (q, k, v) in enumerate(windows(i, c)):
            scores = product(split(q), split(k), 1, 1)
            scores = jnp.where(column < length, scores, MASKED)
            expon = jnp.exp(scores - jnp.max(scores, axis=-1, keepdims=True))
            probs = split(expon / jnp.sum(expon, axis=-1, keepdims=True))
            probs_hi[i, c, h], probs_lo[i, c, h] = probs
            outs.append(product_apart(probs, split(v), 1, 0))
        joined[i, c] = jnp.concatenate([swap(outs[2]), outs[0] + outs[1]], axis=1)
        mid[i] += product(split(joined[i, c]), weight(c, 4 * LANES, attn), 1, 1)
        return 0

    lax.fori_loop(0, 2 * own, attend, 0)
    gather_end(1)
    convert(up, end)

    def feed(t, _):
        i, c = t // 2, t % 2

        @pl.when(c == 0)
        def _():
            second, _ = normalize(mid[i])
            so_hi[i], so_lo[i] = split(second * vec(3) + vec(4))
            yb[i] = mid[i] + vec(5)
            back[i] = jnp.zeros((rows, width), f32)

        so = (so_hi[i], so_lo[i])
        co = (cot_hi[i], cot_lo[i])
        hidden = product(so, weight(c, up, down), 1, 0) + hidden_bias[c]
        portion = 0.5 * (1.0 + lax.erf(hidden * (0.5 ** 0.5)))
        active = split(hidden * portion)
        slope = portion + hidden * jnp.exp(-0.5 * hidden * hidden) * 0.3989422804014327
        yb[i] += product(active, weight(c, down, end), 1, 1)
        buf[c, :, down:end] += product(co, active, 0, 0)
        grad = product(co, weight(c, down, end), 1, 0) * slope
        small_grads[c, 7:8, 0:hidden_local] += total(grad)
        grad = split(grad)
        buf[c, :, up:down] += product(so, grad, 0, 0)
        back[i] += product(grad, weight(c, up, down), 1, 1)

        @pl.when(c == 1)
        def _():
            cot = cots[i]
            second, second_inverse = normalize(mid[i])
            grad_second = back[i]
            small_grads[0, 3:4, 0:width] += total(grad_second * second)
            small_grads[0, 4:5, 0:width] += total(grad_second)
            small_grads[0, 5:6, 0:width] += total(cot)
            grad_middle = cot + norm_back(grad_second, second, second_inverse, vec(3))
            small_grads[0, 2:3, 0:width] += total(grad_middle)
            gm_hi[i], gm_lo[i] = split(grad_middle)
            back[i] = grad_middle
            mid[i] = jnp.zeros((rows, width), f32)
            keep, give, _ = image_copies(0, yb, y_ref, i)
            keep.start()
            give.start()

        return 0

    lax.fori_loop(0, 2 * own, feed, 0)

    scatter_start(1)
    scatter_plan = list(zip(spread(len(back_order) - 1, 2 * own, 1), back_order[:-1]))

    def attend_back(t, _):
        i, c = t // 2, t % 2
        serve(t, scatter_plan, scatter_event)
        gm = (gm_hi[i], gm_lo[i])
        fo = (fo_hi[i], fo_lo[i])
        grad_heads = product(gm, weight(c, 4 * LANES, attn), 1, 0)
        buf[c, :, 4 * LANES:attn] += product(gm, split(joined[i, c]), 0, 0)
        pair, single = grad_heads[:, LANES:], swap(grad_heads[:, :LANES])
        pair_out, single_out = joined[i, c, :, LANES:], swap(joined[i, c, :, :LANES])
        grad_outs = (side(pair, 0), side(pair, 1), side(single, 0))
        outs = (pair_out, pair_out, single_out)
        grads = []
        for h, (q, k, v) in enumerate(windows(i, c)):
            grad_out = grad_outs[h]
            row = jnp.sum(grad_out * outs[h], axis=-1, keepdims=True)
            grad_out = split(grad_out)
            grad_probs = product(grad_out, split(v), 1, 1)
            probs = (probs_hi[i, c, h], probs_lo[i, c, h])
            grad_v = product_apart(probs, grad_out, 0, 0)
            grad_scores = split((probs[0].astype(f32) + probs[1].astype(f32)) * (grad_probs - row))
            grad_q = product_apart(grad_scores, split(k), 1, 0) * score_scale
            grad_k = product_apart(grad_scores, split(q), 0, 0)
            grads.append((grad_q, grad_k, grad_v))
        one, two, three = grads
        grad_mixed = jnp.concatenate(
            [one[0] + two[0], one[1] + two[1], one[2] + two[2], three[0] + swap(three[1]), three[2]], axis=1)
        small_grads[c, 6:7, 0:qkv] += total(grad_mixed)
        grad_mixed = split(grad_mixed)
        buf[c, :, 0:qkv] += product(fo, grad_mixed, 0, 0)
        mid[i] += product(grad_mixed, weight(c, 0, qkv), 1, 1)

        @pl.when(c == 1)
        def _():
            first, first_inverse = normalize(xs[i])
            grad_first = mid[i]
            small_grads[0, 0:1, 0:width] += total(grad_first * first)
            small_grads[0, 1:2, 0:width] += total(grad_first)
            xs[i] = back[i] + norm_back(grad_first, first, first_inverse, vec(0))
            keep, give, _ = image_copies(1, xs, gx_ref, i)
            keep.start()
            give.start()

        return 0

    lax.fori_loop(0, 2 * own, attend_back, 0)

    bias = moved(jnp.concatenate([small_grads[c, 6:7, 0:qkv] for c in range(2)], axis=0), mixed_hot[...], 1)
    hidden = [moved(jnp.concatenate([small_grads[c, 7:8, :] for c in range(2)], axis=0), hidden_hot[half], 1)
              for half in range(2)]
    six = small_grads[0, 0:6, 0:width]
    for c in range(2):
        packed = jnp.concatenate([six, bias[c:c + 1], hidden[0][c:c + 1], hidden[1][c:c + 1],
                                  jnp.zeros((LANES - 9, width), f32)], axis=0)
        buf[c, :, small:up] = packed.T
    scatter_start(0)
    for slab in back_order:
        if slab == back_order[-first_size]:
            scatter_event(1, back_order[-1])
        scatter_event(0, slab)
    for t, source, ref in ((0, yb, y_ref), (1, xs, gx_ref)):
        for i in range(own):
            keep, give, take = image_copies(t, source, ref, i)
            keep.wait()
            give.wait_send()
            take.wait_recv()
    scatter_end(1)
    scatter_end(0)


def run_step(mixer, turned, small, up, down, inputs, cotangent, n, heads, head, length):
    sizes = rings(n)
    width = inputs.shape[1]
    images = inputs.shape[0] // length
    own = images // 2
    rows = -(-length // 16) * 16
    share, hidden_local = up.shape
    columns = 7 * LANES + 2 * hidden_local
    anywhere = pl.BlockSpec(memory_space=pl.ANY)
    act = pltpu.VMEM((own, rows, width), bf16)
    full = pltpu.VMEM((own, rows, width), f32)
    dma = pltpu.SemaphoreType.DMA
    probs = pltpu.VMEM((own, 2, heads, rows, rows), bf16)
    return pl.pallas_call(
        functools.partial(step_kernel, sizes, length, heads, head),
        out_shape=[jax.ShapeDtypeStruct((share, columns), f32), jax.ShapeDtypeStruct((images, rows, width), f32),
                   jax.ShapeDtypeStruct((images, rows, width), f32)],
        in_specs=[pl.BlockSpec(memory_space=pltpu.VMEM)] * 5 + [anywhere] * 2,
        out_specs=[pl.BlockSpec(memory_space=pltpu.VMEM), anywhere, anywhere],
        scratch_shapes=[
            pltpu.VMEM((share, columns), f32),
            pltpu.VMEM((2, width, columns), f32),
            pltpu.VMEM((2, width, columns), bf16), pltpu.VMEM((2, width, columns), bf16),
            full, full, act, act, act, act, act, act, act, act,
            pltpu.VMEM((own, 2, rows, 5 * LANES), f32), probs, probs,
            pltpu.VMEM((own, 2, rows, 2 * LANES), f32), full, full, full,
            pltpu.VMEM((width // LANES, inputs.shape[0], LANES), f32),
            pltpu.VMEM((8, width), f32), pltpu.VMEM((2, 1, 5 * LANES), f32), pltpu.VMEM((2, 1, hidden_local), f32),
            pltpu.VMEM((2, 8, hidden_local), f32),
            pltpu.VMEM((width, 5 * LANES), bf16), pltpu.VMEM((2, width, hidden_local), bf16),
            pltpu.VMEM((n, share, columns), f32), pltpu.VMEM((n - 1, share, columns), f32),
            dma((2, 3, n)), dma((2, n)), dma((2, n)), dma((2, n)),
            dma((2, n)), dma((2, n)), dma((2, n)), dma((2, n)),
            dma((width // LANES,)), dma((2, own)), dma((2, own)), dma((2, own)),
        ],
        compiler_params=pltpu.CompilerParams(
            collective_id=2, has_side_effects=True, vmem_limit_bytes=67043328),
        name="step",
    )(mixer, turned, small, up, down, inputs, cotangent)


def pack_attention(mixer, output):
    head = mixer.shape[2] // 3
    pair = 2 * head
    out = output.T
    q, k, v = mixer[:, 0], mixer[:, 1], mixer[:, 2]
    return jnp.concatenate([q[:, :pair], k[:, :pair], v[:, :pair], q[:, pair:], k[:, pair:], v[:, pair:],
                            out[:, pair:], out[:, :pair]], axis=1)


def unpack_attention(block, head):
    pair = 2 * head
    cut = [block[:, t * head:(t + 1) * head] for t in range(12)]
    mixer = jnp.stack([jnp.concatenate(t, axis=1) for t in (
        (cut[0], cut[1], cut[6]), (cut[2], cut[3], cut[7]), (cut[4], cut[5], cut[8]))], axis=1)
    output = jnp.concatenate([cut[10], cut[11], cut[9]], axis=1).T
    return mixer, output


SMALL = ("first_gain", "first_shift", "output_bias", "second_gain", "second_shift", "reduce_bias",
         "mixer_bias", "expand_bias")


def pack_small(values):
    return jnp.concatenate([values[name].reshape(-1) for name in SMALL])


def unpack_small(flat, like):
    out, start = {}, 0
    for name in SMALL:
        size = like[name].size
        out[name] = flat[start:start + size].reshape(like[name].shape)
        start += size
    return out


def adam_update(param, grad, momentum, variance, decay):
    momentum_next = beta_one * momentum + (1.0 - beta_one) * grad
    variance_next = beta_two * variance + (1.0 - beta_two) * grad * grad
    mean_hat = momentum_next / (1.0 - beta_one**step_count)
    square_hat = variance_next / (1.0 - beta_two**step_count)
    stepped = param - learn_rate * (mean_hat / (jnp.sqrt(square_hat) + adam_eps) + decay * param)
    return (stepped, momentum_next, variance_next)


NAMES = ("first_gain", "first_shift", "mixer_weight", "mixer_bias", "output_weight", "output_bias", "second_gain",
         "second_shift", "expand_weight", "expand_bias", "reduce_weight", "reduce_bias")
DECAYED = ("mixer_weight", "output_weight", "expand_weight", "reduce_weight")


def per_device(inputs, cotangent, *rest):
    if rest[0].shape[0] % 8 == 0:
        return one_kernel(inputs, cotangent, *rest)
    return three_kernels(inputs, cotangent, *rest)


def finish(params, momenta, variances, gradients, block_out, input_gradient):
    results = [adam_update(params[m], gradients[m], momenta[m], variances[m], weight_decay if m in DECAYED else 0.0)
               for m in NAMES]
    return (block_out, input_gradient, *(gradients[m] for m in NAMES), *(r[0] for r in results),
            *(r[1] for r in results), *(r[2] for r in results))


def one_kernel(inputs, cotangent, *rest):
    n = lax.axis_size("dp")
    images, length, width = inputs.shape
    scale = (n * images * length) ** (-0.5)
    params = dict(zip(NAMES, rest[:12]))
    momenta = dict(zip(NAMES, rest[12:24]))
    variances = dict(zip(NAMES, rest[24:]))
    share = params["first_gain"].shape[0]
    heads, piece = params["mixer_bias"].shape[1:]
    head = piece * n
    hidden_local = params["expand_weight"].shape[1]
    small = jnp.pad(pack_small(params).reshape(-1, share).T, ((0, 0), (0, LANES - 9)))
    def tokens(v):
        return v.transpose(1, 0, 2).reshape(length * images, width)

    summed, block_out, input_gradient = run_step(
        params["mixer_weight"].transpose(1, 0, 2), params["output_weight"].T, small, params["expand_weight"],
        params["reduce_weight"].T, tokens(inputs), tokens(cotangent), n, heads, head, length)
    summed = summed * scale
    mixer, output = unpack_attention(summed[:, :6 * LANES], head)
    gradients = unpack_small(summed[:, 6 * LANES:6 * LANES + 9].T.reshape(-1), params)
    up = 7 * LANES
    gradients.update(mixer_weight=mixer, output_weight=output, expand_weight=summed[:, up:up + hidden_local],
                     reduce_weight=summed[:, up + hidden_local:].T)
    return finish(params, momenta, variances, gradients, block_out[:, :length], input_gradient[:, :length])


def three_kernels(inputs, cotangent, *rest):
    n = lax.axis_size("dp")
    scale = (n * inputs.shape[0] * inputs.shape[1]) ** (-0.5)
    params = dict(zip(NAMES, rest[:12]))
    momenta = dict(zip(NAMES, rest[12:24]))
    variances = dict(zip(NAMES, rest[24:]))
    share, width = params["first_gain"].shape[0], inputs.shape[2]
    heads, piece = params["mixer_bias"].shape[1:]
    head = piece * n
    hidden_local = params["expand_weight"].shape[1]
    end = 6 * LANES + 2 * hidden_local

    small = pack_small(params)
    count = small.shape[0]
    slab = jnp.concatenate([
        pack_attention(params["mixer_weight"], params["output_weight"]),
        params["expand_weight"], params["reduce_weight"].T,
        jnp.pad(small, (0, share * LANES - count)).reshape(share, LANES)], axis=1)
    columns = slab.shape[1]
    gathered = gather(slab, n)

    flat = gathered[:, :, :, end:].reshape(2, n, share * LANES)[:, :, :count]
    vectors = jnp.pad(flat[0, :, :6 * share].reshape(n, 6, share).transpose(1, 0, 2).reshape(6, width),
                      ((0, 2), (0, 0)))
    bias = flat[:, :, 6 * share:7 * share].reshape(2, n, 2, heads, piece).transpose(0, 2, 3, 1, 4)
    bias = bias.reshape(2, 2, heads * head)
    q, v, none = bias[:, 0], bias[:, 1], jnp.zeros((2, 2 * head), f32)
    mixed_bias = jnp.concatenate([q[:, :2 * head], none, v[:, :2 * head], q[:, 2 * head:], none[:, :head],
                                  v[:, 2 * head:], none[:, :head]], axis=1)[:, None]
    expand_bias = flat[:, :, 7 * share:].reshape(2, n, -1, piece).transpose(0, 2, 1, 3).reshape(2, 1, -1)

    base = (lax.axis_index("mp") * (inputs.shape[0] // 2)).astype(jnp.int32).reshape(1)
    block_out, input_gradient, grads, small_grads = run_layer(
        base, inputs, cotangent, gathered.reshape(2, width, columns), vectors, mixed_bias, expand_bias, heads, head)

    total = small_grads[:1, :6, :width].reshape(6, n, share).transpose(1, 0, 2).reshape(n, 6 * share)
    row = small_grads[:, 6, :5 * LANES]
    bias = jnp.stack([
        jnp.concatenate([row[:, :2 * head], row[:, 6 * head:7 * head]], axis=1),
        jnp.concatenate([row[:, 4 * head:6 * head], row[:, 8 * head:9 * head]], axis=1)], axis=1)
    bias = bias.reshape(2, 2, heads, n, piece).transpose(0, 3, 1, 2, 4).reshape(2, n, share)
    hidden = small_grads[:, 7].reshape(2, hidden_local // head, n, piece).transpose(0, 2, 1, 3).reshape(2, n, -1)
    packed = jnp.concatenate([jnp.broadcast_to(total[None], (2,) + total.shape), bias, hidden], axis=2)
    packed = jnp.pad(packed, ((0, 0), (0, 0), (0, share * LANES - count))).reshape(2, n, share, LANES)
    grads = lax.dynamic_update_slice(grads.reshape(2, n, share, columns), packed, (0, 0, 0, end))

    summed, block_out, input_gradient = scatter(grads, block_out, input_gradient, n)
    summed = summed * scale
    mixer, output = unpack_attention(summed[:, :6 * LANES], head)
    gradients = unpack_small(summed[:, end:].reshape(-1), params)
    gradients.update(mixer_weight=mixer, output_weight=output,
                     expand_weight=summed[:, 6 * LANES:6 * LANES + hidden_local],
                     reduce_weight=summed[:, 6 * LANES + hidden_local:end].T)
    return finish(params, momenta, variances, gradients, block_out, input_gradient)


def solution(mesh):
    images = P("dp", None, None)
    entries = (P("dp"), P("dp"), P("dp", None, "mp"), P(None, "mp", "dp"), P("mp", "dp"), P("dp"), P("dp"), P("dp"),
               P("dp", "mp"), P("mp", "dp"), P("mp", "dp"), P("dp"))
    return jax.shard_map(per_device, mesh=mesh, in_specs=(images, images) + entries * 3,
                         out_specs=(images, images) + entries * 4, check_vma=False)
```
